8 devices in a mesh: dp: 2 (over y, z), tp: 4 (over x, core).
Axes of the slice: x: 2, y: 2, z: 1, core: 2. Of those that a mesh axis runs over, the one named last changes fastest.
Arguments:
- x: bfloat16 [4096, 2048], P(('dp', 'tp')), parts along dimension 0
- w_gate: bfloat16 [2048, 8192], P(None, 'tp')
- w_up: bfloat16 [2048, 8192], P(None, 'tp')
- w_down: bfloat16 [8192, 2048], P('tp')
Outputs:
- output: bfloat16 [4096, 2048], P(('dp', 'tp')), parts along dimension 0
There are 2 independent parts. The reference program is written for one: setup_inputs(seed, part) draws one part's arguments, and reference() takes and returns one part's arrays. A program takes and returns all parts, laid end to end along the dimension named above; an argument that names none is the same for every part.
All inputs are finite; a program needn't handle non-finite values.
Results may differ from the reference program's by a relative error of at most 0.016.
Values are sent between devices in bfloat16 or wider.
A program may use at most 2 GiB of HBM per device.

```python
import jax
import jax.numpy as jnp

ROWS = 2048
D = 2048
FF = 8192


def setup_inputs(seed: int = 0, part: int = 0) -> dict:
    kx, kg, ku, kd = jax.random.split(jax.random.key(seed), 4)
    drawn = {
        "x": jax.random.normal(jax.random.fold_in(kx, part), (ROWS, D), jnp.float32),
        "w_gate": jax.random.normal(kg, (D, FF), jnp.float32) * D**-0.5,
        "w_up": jax.random.normal(ku, (D, FF), jnp.float32) * D**-0.5,
        "w_down": jax.random.normal(kd, (FF, D), jnp.float32) * FF**-0.5,
    }
    return {k: v.astype(jnp.bfloat16) for k, v in drawn.items()}


def reference(x, w_gate, w_up, w_down):
    gate = jnp.dot(x, w_gate, preferred_element_type=jnp.float32)
    up = jnp.dot(x, w_up, preferred_element_type=jnp.float32)
    hidden = (jax.nn.silu(gate) * up).astype(jnp.bfloat16)
    return jnp.dot(hidden, w_down, preferred_element_type=jnp.float32).astype(jnp.bfloat16)
```

```python
import jax
import jax.numpy as jnp
from jax import lax
from jax.experimental import pallas as pl
from jax.experimental.pallas import tpu as pltpu
from jax.sharding import PartitionSpec as P

BF16, F32 = jnp.bfloat16, jnp.float32
MESH = pl.DeviceIdType.MESH

HALF = 128
M = 2 * HALF
NT = 512
BLK = 32

ORDER = (("L", 0), ("L", 1), ("L", 2), ("R", 0), ("R", 1), ("L", 3), ("R", 2), ("R", 3))
FORWARD_MID = {1: 0, 4: 2, 5: 3}
FORWARD_END = {2: 1}


def kernel(
    x, w_gate, w_up, w_down, out,
    xs, wg, wu, wd, hid, term, local, to_sib, from_sib, to_far, from_far, done,
    own_sem, w_sem, sib_send, sib_recv, far_send, far_recv, fwd_send, fwd_recv,
    term_send, term_recv, sum_send, sum_recv, out_sem,
):
    me = lax.axis_index("tp")
    sib = me + 1 - 2 * lax.rem(me, 2)
    far = lax.rem(me + 2, 4)
    steps = len(ORDER)
    tiles = wg.shape[0]
    dtiles = wd.shape[0]
    slot = {k: s for s, k in enumerate(ORDER)}
    chunks = x.shape[0] // HALF

    mine, other = pl.ds(0, HALF), pl.ds(HALF, HALF)

    def remote(src, dst, send, recv, tp):
        return pltpu.make_async_remote_copy(
            src_ref=src, dst_ref=dst, send_sem=send, recv_sem=recv,
            device_id={"tp": tp}, device_id_type=MESH)

    def own(j):
        return pltpu.make_async_copy(x.at[pl.ds(j * HALF, HALF)], xs.at[slot["L", j], mine], own_sem.at[j])

    def to_sibling(j):
        return remote(x.at[pl.ds(j * HALF, HALF)], xs.at[slot["L", j], other], sib_send.at[j], sib_recv.at[j], sib)

    def to_far_chip(j):
        return remote(x.at[pl.ds(j * HALF, HALF)], xs.at[slot["R", j], mine], far_send.at[j], far_recv.at[j], far)

    def forward(i):
        s = slot["R", i]
        return remote(xs.at[s, mine], xs.at[s, other], fwd_send.at[i], fwd_recv.at[i], sib)

    def term_copy(s):
        return remote(to_sib.at[s], from_sib.at[s], term_send.at[s], term_recv.at[s], sib)

    def sum_copy(i, b):
        rows = pl.ds(i * HALF + b * BLK, BLK)
        k = i * (HALF // BLK) + b
        return remote(to_far.at[rows], from_far.at[rows], sum_send.at[k], sum_recv.at[k], far)

    def weights(n):
        c = pl.ds(n * NT, NT)
        return (pltpu.make_async_copy(w_gate.at[:, c], wg.at[n], w_sem.at[0, n]),
                pltpu.make_async_copy(w_up.at[:, c], wu.at[n], w_sem.at[1, n]))

    def weights_down(n):
        return pltpu.make_async_copy(w_down.at[:, pl.ds(n * NT, NT)], wd.at[n], w_sem.at[2, n])

    def out_copy(i, b):
        rows = pl.ds(i * HALF + b * BLK, BLK)
        k = i * (HALF // BLK) + b
        return pltpu.make_async_copy(done.at[rows], out.at[rows], out_sem.at[k])

    barrier = pltpu.get_barrier_semaphore()
    for d in (sib, far):
        pl.semaphore_signal(barrier, inc=1, device_id={"tp": d}, device_id_type=MESH)
    own(0).start()
    for n in range(tiles):
        for c in weights(n):
            c.start()
    pl.semaphore_wait(barrier, 2)
    for j in range(chunks):
        to_far_chip(j).start()
    for j in range(chunks):
        to_sibling(j).start()
    for n in range(dtiles):
        weights_down(n).start()
    for j in range(1, chunks):
        own(j).start()

    def round_term(s):
        def blk(r, _):
            rows = pl.ds(pl.multiple_of(r * BLK, BLK), BLK)
            to_sib[s, rows] = term[lax.rem(s, 2), pl.ds(pl.multiple_of(HALF + r * BLK, BLK), BLK)].astype(BF16)
            return 0
        lax.fori_loop(0, HALF // BLK, blk, 0)

    def chip_sum(s):
        term_copy(s).wait_recv()
        kind, i = ORDER[s]

        def blk(r, _):
            rows = pl.ds(pl.multiple_of(r * BLK, BLK), BLK)
            both = term[s % 2, rows] + from_sib[s, rows].astype(F32)
            at = pl.ds(pl.multiple_of(i * HALF + r * BLK, BLK), BLK)
            if kind == "L":
                local[at] = both
            else:
                to_far[at] = both.astype(BF16)
            return 0
        lax.fori_loop(0, HALF // BLK, blk, 0)

    def start_sum(s):
        kind, i = ORDER[s]
        if kind == "R":
            for b in range(HALF // BLK):
                sum_copy(i, b).start()

    def step(s, _):
        for k, (kind, i) in enumerate(ORDER):
            @pl.when(s == k)
            def _():
                if kind == "L":
                    own(i).wait()
                    to_sibling(i).wait_recv()
                else:
                    forward(i).wait_recv()

        def gate_up(n, _):
            @pl.when(s == 0)
            def _():
                c = pl.ds(0, NT)
                pltpu.make_async_copy(w_gate.at[:, c], wg.at[n], w_sem.at[0, n]).wait()
                pltpu.make_async_copy(w_up.at[:, c], wu.at[n], w_sem.at[1, n]).wait()

            gate = jnp.dot(xs[s], wg[n], preferred_element_type=F32)
            up = jnp.dot(xs[s], wu[n], preferred_element_type=F32)
            hid[:, pl.ds(pl.multiple_of(n * NT, NT), NT)] = (jax.nn.silu(gate) * up).astype(BF16)

            @pl.when((n == 0) & (s > 0))
            def _():
                p = s - 1
                remote(to_sib.at[p], from_sib.at[p], term_send.at[p], term_recv.at[p], sib).start()
            return 0

        lax.fori_loop(0, tiles, gate_up, 0)

        for k, i in FORWARD_MID.items():
            @pl.when(s == k)
            def _():
                to_far_chip(i).wait_recv()
                forward(i).start()
        for k in range(1, steps):
            @pl.when(s == k)
            def _():
                chip_sum(k - 1)

        def down(n, _):
            @pl.when(s == 0)
            def _():
                pltpu.make_async_copy(w_down.at[:, pl.ds(0, NT)], wd.at[n], w_sem.at[2, n]).wait()

            cols = pl.ds(pl.multiple_of(n * NT, NT), NT)
            term[lax.rem(s, 2), :, cols] = jnp.dot(hid[...], wd[n], preferred_element_type=F32)
            return 0

        lax.fori_loop(0, dtiles, down, 0)

        round_term(s)
        for k, i in FORWARD_END.items():
            @pl.when(s == k)
            def _():
                to_far_chip(i).wait_recv()
                forward(i).start()
        for k in range(1, steps):
            if ORDER[k - 1][0] == "R":
                @pl.when(s == k)
                def _():
                    start_sum(k - 1)
        return 0

    lax.fori_loop(0, steps, step, 0)

    def finish(i, b):
        sum_copy(i, b).wait_recv()
        rows = pl.ds(i * HALF + b * BLK, BLK)
        done[rows] = (local[rows] + from_far[rows].astype(F32)).astype(BF16)
        out_copy(i, b).start()

    last = steps - 1
    term_copy(last).start()
    blocks = HALF // BLK
    for b in range(blocks):
        finish(0, b)
    chip_sum(last)
    for b in range(blocks):
        finish(1, b)
    start_sum(last)
    for i in range(2, chunks):
        for b in range(blocks):
            finish(i, b)

    for j in range(chunks):
        to_far_chip(j).wait_send()
        to_sibling(j).wait_send()
        forward(j).wait_send()
    for s in range(steps):
        term_copy(s).wait_send()
    for i in range(chunks):
        for b in range(blocks):
            sum_copy(i, b).wait_send()
            out_copy(i, b).wait()


def solution(mesh):
    def step(x, w_gate, w_up, w_down):
        rows, d = x.shape
        f = w_gate.shape[1]
        chunks = rows // HALF
        steps = len(ORDER)
        sums = chunks * (HALF // BLK)
        dma = pltpu.SemaphoreType.DMA
        return pl.pallas_call(
            kernel,
            out_shape=jax.ShapeDtypeStruct((rows, d), BF16),
            in_specs=[pl.BlockSpec(memory_space=pl.ANY)] * 4,
            out_specs=pl.BlockSpec(memory_space=pl.ANY),
            scratch_shapes=[
                pltpu.VMEM((steps, M, d), BF16),
                pltpu.VMEM((f // NT, d, NT), BF16),
                pltpu.VMEM((f // NT, d, NT), BF16),
                pltpu.VMEM((d // NT, f, NT), BF16),
                pltpu.VMEM((M, f), BF16),
                pltpu.VMEM((2, M, d), F32),
                pltpu.VMEM((rows, d), F32),
                pltpu.VMEM((steps, HALF, d), BF16),
                pltpu.VMEM((steps, HALF, d), BF16),
                pltpu.VMEM((rows, d), BF16),
                pltpu.VMEM((rows, d), BF16),
                pltpu.VMEM((rows, d), BF16),
                dma((chunks,)),
                dma((3, f // NT)),
                dma((chunks,)), dma((chunks,)),
                dma((chunks,)), dma((chunks,)),
                dma((chunks,)), dma((chunks,)),
                dma((steps,)), dma((steps,)),
                dma((sums,)), dma((sums,)),
                dma((sums,)),
            ],
            compiler_params=pltpu.CompilerParams(
                collective_id=0, has_side_effects=True, vmem_limit_bytes=67000000),
            name="mlp_ring",
        )(x, w_gate, w_up, w_down)

    return jax.shard_map(
        step,
        mesh=mesh,
        in_specs=(P(("dp", "tp"), None), P(None, "tp"), P(None, "tp"), P("tp", None)),
        out_specs=P(("dp", "tp"), None),
        check_vma=False,
    )
```

```python
import jax
import jax.numpy as jnp
from jax import lax
from jax.experimental import pallas as pl
from jax.experimental.pallas import tpu as pltpu
from jax.sharding import PartitionSpec as P

BF16, F32 = jnp.bfloat16, jnp.float32
MESH = pl.DeviceIdType.MESH

HALF = 128
M = 2 * HALF
NT = 512
BLK = 32

ORDER = (("L", 0), ("L", 1), ("L", 2), ("R", 0), ("R", 1), ("L", 3), ("R", 2), ("R", 3))
FORWARD_MID = {1: 0, 4: 2, 5: 3}
FORWARD_END = {2: 1}


def kernel(
    x, w_gate, w_up, w_down, out,
    xs, wg, wu, wd, hid, term, local, to_sib, from_sib, to_far, from_far,
    own_sem, w_sem, sib_send, sib_recv, far_send, far_recv, fwd_send, fwd_recv,
    term_send, term_recv, sum_send, sum_recv,
):
    me = lax.axis_index("tp")
    sib = me + 1 - 2 * lax.rem(me, 2)
    far = lax.rem(me + 2, 4)
    steps = len(ORDER)
    tiles = wg.shape[0]
    dtiles = wd.shape[0]
    slot = {k: s for s, k in enumerate(ORDER)}
    chunks = x.shape[0] // HALF

    mine, other = pl.ds(0, HALF), pl.ds(HALF, HALF)

    def remote(src, dst, send, recv, tp):
        return pltpu.make_async_remote_copy(
            src_ref=src, dst_ref=dst, send_sem=send, recv_sem=recv,
            device_id={"tp": tp}, device_id_type=MESH)

    def own(j):
        return pltpu.make_async_copy(x.at[pl.ds(j * HALF, HALF)], xs.at[slot["L", j], mine], own_sem.at[j])

    def to_sibling(j):
        return remote(xs.at[slot["L", j], mine], xs.at[slot["L", j], other], sib_send.at[j], sib_recv.at[j], sib)

    def to_far_chip(j):
        return remote(xs.at[slot["L", j], mine], xs.at[slot["R", j], mine], far_send.at[j], far_recv.at[j], far)

    def forward(i):
        s = slot["R", i]
        return remote(xs.at[s, mine], xs.at[s, other], fwd_send.at[i], fwd_recv.at[i], sib)

    def term_copy(s):
        return remote(to_sib.at[s], from_sib.at[s], term_send.at[s], term_recv.at[s], sib)

    def sum_copy(i, b):
        rows = pl.ds(i * HALF + b * BLK, BLK)
        k = i * (HALF // BLK) + b
        return remote(to_far.at[rows], from_far.at[rows], sum_send.at[k], sum_recv.at[k], far)

    def weights(n):
        c = pl.ds(n * NT, NT)
        return (pltpu.make_async_copy(w_gate.at[:, c], wg.at[n], w_sem.at[0, n]),
                pltpu.make_async_copy(w_up.at[:, c], wu.at[n], w_sem.at[1, n]))

    def weights_down(n):
        return pltpu.make_async_copy(w_down.at[:, pl.ds(n * NT, NT)], wd.at[n], w_sem.at[2, n])

    def out_copy(i, b):
        rows = pl.ds(i * HALF + b * BLK, BLK)
        k = i * (HALF // BLK) + b
        return pltpu.make_async_copy(done.at[rows], out.at[rows], out_sem.at[k])

    barrier = pltpu.get_barrier_semaphore()
    for d in (sib, far):
        pl.semaphore_signal(barrier, inc=1, device_id={"tp": d}, device_id_type=MESH)
    for j in range(chunks):
        own(j).start()
    for j in range(chunks):
        own(j).wait()
    pl.semaphore_wait(barrier, 2)
    for j in range(chunks):
        to_far_chip(j).start()
    for j in range(chunks):
        to_sibling(j).start()
    for n in range(tiles):
        for c in weights(n):
            c.start()
    for n in range(dtiles):
        weights_down(n).start()

    def round_term(s):
        def blk(r, _):
            rows = pl.ds(pl.multiple_of(r * BLK, BLK), BLK)
            to_sib[s, rows] = term[lax.rem(s, 2), pl.ds(pl.multiple_of(HALF + r * BLK, BLK), BLK)].astype(BF16)
            return 0
        lax.fori_loop(0, HALF // BLK, blk, 0)

    def chip_sum(s):
        term_copy(s).wait_recv()
        kind, i = ORDER[s]

        def blk(r, _):
            rows = pl.ds(pl.multiple_of(r * BLK, BLK), BLK)
            both = term[s % 2, rows] + from_sib[s, rows].astype(F32)
            at = pl.ds(pl.multiple_of(i * HALF + r * BLK, BLK), BLK)
            if kind == "L":
                local[at] = both
            else:
                to_far[at] = both.astype(BF16)
            return 0
        lax.fori_loop(0, HALF // BLK, blk, 0)

    def start_sum(s):
        kind, i = ORDER[s]
        if kind == "R":
            for b in range(HALF // BLK):
                sum_copy(i, b).start()

    def step(s, _):
        for k, (kind, i) in enumerate(ORDER):
            @pl.when(s == k)
            def _():
                if kind == "L":
                    to_sibling(i).wait_recv()
                else:
                    forward(i).wait_recv()

        def gate_up(n, _):
            @pl.when(s == 0)
            def _():
                c = pl.ds(0, NT)
                pltpu.make_async_copy(w_gate.at[:, c], wg.at[n], w_sem.at[0, n]).wait()
                pltpu.make_async_copy(w_up.at[:, c], wu.at[n], w_sem.at[1, n]).wait()

            gate = jnp.dot(xs[s], wg[n], preferred_element_type=F32)
            up = jnp.dot(xs[s], wu[n], preferred_element_type=F32)
            hid[:, pl.ds(pl.multiple_of(n * NT, NT), NT)] = (jax.nn.silu(gate) * up).astype(BF16)

            @pl.when((n == 0) & (s > 0))
            def _():
                p = s - 1
                remote(to_sib.at[p], from_sib.at[p], term_send.at[p], term_recv.at[p], sib).start()
            return 0

        lax.fori_loop(0, tiles, gate_up, 0)

        for k, i in FORWARD_MID.items():
            @pl.when(s == k)
            def _():
                to_far_chip(i).wait_recv()
                forward(i).start()
        for k in range(1, steps):
            @pl.when(s == k)
            def _():
                chip_sum(k - 1)

        def down(n, _):
            @pl.when(s == 0)
            def _():
                pltpu.make_async_copy(w_down.at[:, pl.ds(0, NT)], wd.at[n], w_sem.at[2, n]).wait()

            cols = pl.ds(pl.multiple_of(n * NT, NT), NT)
            term[lax.rem(s, 2), :, cols] = jnp.dot(hid[...], wd[n], preferred_element_type=F32)
            return 0

        lax.fori_loop(0, dtiles, down, 0)

        round_term(s)
        for k, i in FORWARD_END.items():
            @pl.when(s == k)
            def _():
                to_far_chip(i).wait_recv()
                forward(i).start()
        for k in range(1, steps):
            if ORDER[k - 1][0] == "R":
                @pl.when(s == k)
                def _():
                    start_sum(k - 1)
        return 0

    lax.fori_loop(0, steps, step, 0)

    def finish(i, b):
        sum_copy(i, b).wait_recv()
        rows = pl.ds(i * HALF + b * BLK, BLK)
        out[rows] = (local[rows] + from_far[rows].astype(F32)).astype(BF16)

    last = steps - 1
    term_copy(last).start()
    blocks = HALF // BLK
    for b in range(blocks):
        finish(0, b)
    chip_sum(last)
    for b in range(blocks):
        finish(1, b)
    start_sum(last)
    for i in range(2, chunks):
        for b in range(blocks):
            finish(i, b)

    for j in range(chunks):
        to_far_chip(j).wait_send()
        to_sibling(j).wait_send()
        forward(j).wait_send()
    for s in range(steps):
        term_copy(s).wait_send()
    for i in range(chunks):
        for b in range(blocks):
            sum_copy(i, b).wait_send()


def solution(mesh):
    def step(x, w_gate, w_up, w_down):
        rows, d = x.shape
        f = w_gate.shape[1]
        chunks = rows // HALF
        steps = len(ORDER)
        sums = chunks * (HALF // BLK)
        dma = pltpu.SemaphoreType.DMA
        return pl.pallas_call(
            kernel,
            out_shape=pltpu.VMEM((rows, d), BF16),
            in_specs=[pl.BlockSpec(memory_space=pl.ANY)] * 4,
            out_specs=pl.BlockSpec(memory_space=pltpu.VMEM),
            scratch_shapes=[
                pltpu.VMEM((steps, M, d), BF16),
                pltpu.VMEM((f // NT, d, NT), BF16),
                pltpu.VMEM((f // NT, d, NT), BF16),
                pltpu.VMEM((d // NT, f, NT), BF16),
                pltpu.VMEM((M, f), BF16),
                pltpu.VMEM((2, M, d), F32),
                pltpu.VMEM((rows, d), F32),
                pltpu.VMEM((steps, HALF, d), BF16),
                pltpu.VMEM((steps, HALF, d), BF16),
                pltpu.VMEM((rows, d), BF16),
                pltpu.VMEM((rows, d), BF16),
                dma((chunks,)),
                dma((3, f // NT)),
                dma((chunks,)), dma((chunks,)),
                dma((chunks,)), dma((chunks,)),
                dma((chunks,)), dma((chunks,)),
                dma((steps,)), dma((steps,)),
                dma((sums,)), dma((sums,)),
            ],
            compiler_params=pltpu.CompilerParams(
                collective_id=0, has_side_effects=True, vmem_limit_bytes=63000000),
            name="mlp_ring",
        )(x, w_gate, w_up, w_down)

    return jax.shard_map(
        step,
        mesh=mesh,
        in_specs=(P(("dp", "tp"), None), P(None, "tp"), P(None, "tp"), P("tp", None)),
        out_specs=P(("dp", "tp"), None),
        check_vma=False,
    )
```

```python
import jax
import jax.numpy as jnp
from jax import lax
from jax.experimental import pallas as pl
from jax.experimental.pallas import tpu as pltpu
from jax.sharding import PartitionSpec as P

BF16, F32 = jnp.bfloat16, jnp.float32
MESH = pl.DeviceIdType.MESH

HALF = 128
M = 2 * HALF
NT = 512
BLK = 32
MOVED = 32
KEPT = HALF - MOVED
PIECES = ((0, 0, HALF), (1, 0, HALF), (2, 0, HALF), (3, 0, KEPT), (3, KEPT, MOVED))

ORDER = (("L", 0), ("L", 1), ("R", 0), ("L", 2), ("R", 1), ("R", 2), ("L", 3), ("R", 3))
FORWARD_MID = {1: 0, 4: 2, 5: 3}
FORWARD_END = {2: 1}
LAST = 3


def kernel(
    x, w_gate, w_up, w_down, out,
    xs, wg, wu, wd, hid, term, local, to_sib, from_sib, to_far, from_far,
    own_sem, w_sem, sib_send, sib_recv, far_send, far_recv, fwd_send, fwd_recv,
    extra_sem, term_send, term_recv, sum_send, sum_recv,
):
    me = lax.axis_index("tp")
    core = lax.rem(me, 2)
    sib = me + 1 - 2 * lax.rem(me, 2)
    far = lax.rem(me + 2, 4)
    steps = len(ORDER)
    tiles = wg.shape[0]
    dtiles = wd.shape[0]
    slot = {k: s for s, k in enumerate(ORDER)}
    chunks = x.shape[0] // HALF

    mine, other = pl.ds(0, HALF), pl.ds(HALF, HALF)

    def remote(src, dst, send, recv, tp):
        return pltpu.make_async_remote_copy(
            src_ref=src, dst_ref=dst, send_sem=send, recv_sem=recv,
            device_id={"tp": tp}, device_id_type=MESH)

    def own(j):
        return pltpu.make_async_copy(x.at[pl.ds(j * HALF, HALF)], xs.at[slot["L", j], mine], own_sem.at[j])

    def to_sibling(j):
        return remote(xs.at[slot["L", j], mine], xs.at[slot["L", j], other], sib_send.at[j], sib_recv.at[j], sib)

    def to_far_chip(p):
        j, r, n = PIECES[p]
        rows = pl.ds(r, n)
        return remote(xs.at[slot["L", j], rows], xs.at[slot["R", j], rows], far_send.at[p], far_recv.at[p], far)

    def forward(p):
        i, r, n = PIECES[p]
        s = slot["R", i]
        return remote(xs.at[s, pl.ds(r, n)], xs.at[s, pl.ds(HALF + r, n)], fwd_send.at[p], fwd_recv.at[p], sib)

    moved = pl.ds(HALF + KEPT, MOVED)

    def extra():
        return remote(xs.at[slot["L", LAST], moved], xs.at[slot["R", LAST], moved], extra_sem.at[0], extra_sem.at[1], far)

    def extra_forward():
        s = slot["R", LAST]
        return remote(xs.at[s, moved], xs.at[s, pl.ds(KEPT, MOVED)], extra_sem.at[2], extra_sem.at[3], sib)

    def term_copy(s):
        return remote(to_sib.at[s], from_sib.at[s], term_send.at[s], term_recv.at[s], sib)

    def sum_copy(p):
        i, r, n = PIECES[p]
        rows = pl.ds(i * HALF + r, n)
        return remote(to_far.at[rows], from_far.at[rows], sum_send.at[p], sum_recv.at[p], far)

    def weights(n):
        c = pl.ds(n * NT, NT)
        return (pltpu.make_async_copy(w_gate.at[:, c], wg.at[n], w_sem.at[0, n]),
                pltpu.make_async_copy(w_up.at[:, c], wu.at[n], w_sem.at[1, n]))

    def weights_down(n):
        return pltpu.make_async_copy(w_down.at[:, pl.ds(n * NT, NT)], wd.at[n], w_sem.at[2, n])

    barrier = pltpu.get_barrier_semaphore()
    for d in (sib, far):
        pl.semaphore_signal(barrier, inc=1, device_id={"tp": d}, device_id_type=MESH)
    for j in range(chunks):
        own(j).start()
    own(0).wait()
    pl.semaphore_wait(barrier, 2)
    to_far_chip(0).start()
    for j in range(1, chunks):
        own(j).wait()
        to_far_chip(j).start()

    @pl.when(core == 1)
    def _():
        to_far_chip(4).start()

    for n in range(tiles):
        for c in weights(n):
            c.start()
    for j in range(chunks):
        to_sibling(j).start()
    for n in range(dtiles):
        weights_down(n).start()

    def round_term(s):
        def blk(r, _):
            rows = pl.ds(pl.multiple_of(r * BLK, BLK), BLK)
            to_sib[s, rows] = term[lax.rem(s, 2), pl.ds(pl.multiple_of(HALF + r * BLK, BLK), BLK)].astype(BF16)
            return 0
        lax.fori_loop(0, HALF // BLK, blk, 0)

    def chip_sum(s):
        term_copy(s).wait_recv()
        kind, i = ORDER[s]

        def blk(r, _):
            rows = pl.ds(pl.multiple_of(r * BLK, BLK), BLK)
            both = term[s % 2, rows] + from_sib[s, rows].astype(F32)
            at = pl.ds(pl.multiple_of(i * HALF + r * BLK, BLK), BLK)
            if kind == "L":
                local[at] = both
            else:
                to_far[at] = both.astype(BF16)
            return 0
        lax.fori_loop(0, HALF // BLK, blk, 0)

    def start_sum(s):
        kind, i = ORDER[s]
        if kind == "R":
            for p in range(len(PIECES)):
                if PIECES[p][0] == i:
                    sum_copy(p).start()

    def pass_on(i):
        to_far_chip(i).wait_recv()
        forward(i).start()
        if i == LAST:
            @pl.when(core == 1)
            def _():
                to_far_chip(4).wait_recv()
                forward(4).start()
                extra().wait_recv()
                extra_forward().start()

    def step(s, _):
        for k, (kind, i) in enumerate(ORDER):
            @pl.when(s == k)
            def _():
                if kind == "L":
                    if i != LAST:
                        to_sibling(i).wait_recv()
                else:
                    forward(i).wait_recv()
                    if i == LAST:
                        @pl.when(core == 0)
                        def _():
                            forward(4).wait_recv()
                            extra_forward().wait_recv()

        def gate_up(n, _):
            @pl.when(s == 0)
            def _():
                c = pl.ds(0, NT)
                pltpu.make_async_copy(w_gate.at[:, c], wg.at[n], w_sem.at[0, n]).wait()
                pltpu.make_async_copy(w_up.at[:, c], wu.at[n], w_sem.at[1, n]).wait()

            gate = jnp.dot(xs[s], wg[n], preferred_element_type=F32)
            up = jnp.dot(xs[s], wu[n], preferred_element_type=F32)
            hid[:, pl.ds(pl.multiple_of(n * NT, NT), NT)] = (jax.nn.silu(gate) * up).astype(BF16)

            @pl.when((n == 0) & (s > 0))
            def _():
                p = s - 1
                remote(to_sib.at[p], from_sib.at[p], term_send.at[p], term_recv.at[p], sib).start()
            return 0

        lax.fori_loop(0, tiles, gate_up, 0)

        @pl.when(s == 0)
        def _():
            to_sibling(LAST).wait_recv()

            @pl.when(core == 1)
            def _():
                extra().start()

        for k, i in FORWARD_MID.items():
            @pl.when(s == k)
            def _():
                pass_on(i)
        for k in range(1, steps):
            @pl.when(s == k)
            def _():
                chip_sum(k - 1)

        def down(n, _):
            @pl.when(s == 0)
            def _():
                pltpu.make_async_copy(w_down.at[:, pl.ds(0, NT)], wd.at[n], w_sem.at[2, n]).wait()

            cols = pl.ds(pl.multiple_of(n * NT, NT), NT)
            term[lax.rem(s, 2), :, cols] = jnp.dot(hid[...], wd[n], preferred_element_type=F32)
            for k in range(1, steps):
                if ORDER[k - 1][0] == "R":
                    @pl.when((n == 0) & (s == k))
                    def _():
                        start_sum(k - 1)
            return 0

        lax.fori_loop(0, dtiles, down, 0)

        round_term(s)
        for k, i in FORWARD_END.items():
            @pl.when(s == k)
            def _():
                pass_on(i)
        return 0

    lax.fori_loop(0, steps, step, 0)

    def finish(p):
        sum_copy(p).wait_recv()
        i, r, n = PIECES[p]
        rows = pl.ds(i * HALF + r, n)
        out[rows] = (local[rows] + from_far[rows].astype(F32)).astype(BF16)

    last = steps - 1
    finish(0)
    term_copy(last).start()
    chip_sum(last)
    finish(1)
    start_sum(last)
    for p in range(2, len(PIECES)):
        finish(p)

    for j in range(chunks):
        to_far_chip(j).wait_send()
        to_sibling(j).wait_send()
        forward(j).wait_send()

    @pl.when(core == 1)
    def _():
        to_far_chip(4).wait_send()
        forward(4).wait_send()
        extra().wait_send()
        extra_forward().wait_send()

    for s in range(steps):
        term_copy(s).wait_send()
    for p in range(len(PIECES)):
        sum_copy(p).wait_send()


def solution(mesh):
    def step(x, w_gate, w_up, w_down):
        rows, d = x.shape
        f = w_gate.shape[1]
        chunks = rows // HALF
        steps = len(ORDER)
        pieces = len(PIECES)
        dma = pltpu.SemaphoreType.DMA
        return pl.pallas_call(
            kernel,
            out_shape=pltpu.VMEM((rows, d), BF16),
            in_specs=[pl.BlockSpec(memory_space=pl.ANY)] * 4,
            out_specs=pl.BlockSpec(memory_space=pltpu.VMEM),
            scratch_shapes=[
                pltpu.VMEM((steps, M, d), BF16),
                pltpu.VMEM((f // NT, d, NT), BF16),
                pltpu.VMEM((f // NT, d, NT), BF16),
                pltpu.VMEM((d // NT, f, NT), BF16),
                pltpu.VMEM((M, f), BF16),
                pltpu.VMEM((2, M, d), F32),
                pltpu.VMEM((rows, d), F32),
                pltpu.VMEM((steps, HALF, d), BF16),
                pltpu.VMEM((steps, HALF, d), BF16),
                pltpu.VMEM((rows, d), BF16),
                pltpu.VMEM((rows, d), BF16),
                dma((chunks,)),
                dma((3, f // NT)),
                dma((chunks,)), dma((chunks,)),
                dma((pieces,)), dma((pieces,)),
                dma((pieces,)), dma((pieces,)),
                dma((4,)),
                dma((steps,)), dma((steps,)),
                dma((pieces,)), dma((pieces,)),
            ],
            compiler_params=pltpu.CompilerParams(
                collective_id=0, has_side_effects=True, vmem_limit_bytes=63000000),
            name="mlp_ring",
        )(x, w_gate, w_up, w_down)

    return jax.shard_map(
        step,
        mesh=mesh,
        in_specs=(P(("dp", "tp"), None), P(None, "tp"), P(None, "tp"), P("tp", None)),
        out_specs=P(("dp", "tp"), None),
        check_vma=False,
    )
```

```python
import jax
import jax.numpy as jnp
from jax import lax
from jax.experimental import pallas as pl
from jax.experimental.pallas import tpu as pltpu
from jax.sharding import PartitionSpec as P

BF16, F32 = jnp.bfloat16, jnp.float32
MESH = pl.DeviceIdType.MESH

HALF = 128
M = 2 * HALF
NT = 512
BLK = 32
MOVED = 32
KEPT = HALF - MOVED
PIECES = ((0, 0, HALF), (1, 0, HALF), (2, 0, HALF), (3, 0, KEPT), (3, KEPT, MOVED))

ORDER = (("L", 0), ("L", 1), ("R", 0), ("L", 2), ("R", 1), ("R", 2), ("L", 3), ("R", 3))
FORWARD_MID = {1: 0, 4: 2, 5: 3}
FORWARD_END = {2: 1}
LAST = 3


def kernel(
    x, w_gate, w_up, w_down, out,
    xs, wg, wu, wd, hid, term, local, to_sib, from_sib, to_far, from_far,
    own_sem, w_sem, sib_send, sib_recv, far_send, far_recv, fwd_send, fwd_recv,
    extra_sem, term_send, term_recv, sum_send, sum_recv, sib_in,
):
    me = lax.axis_index("tp")
    core = lax.rem(me, 2)
    sib = me + 1 - 2 * lax.rem(me, 2)
    far = lax.rem(me + 2, 4)
    steps = len(ORDER)
    tiles = wg.shape[0]
    dtiles = wd.shape[0]
    slot = {k: s for s, k in enumerate(ORDER)}
    chunks = x.shape[0] // HALF

    mine, other = pl.ds(0, HALF), pl.ds(HALF, HALF)

    def remote(src, dst, send, recv, tp):
        return pltpu.make_async_remote_copy(
            src_ref=src, dst_ref=dst, send_sem=send, recv_sem=recv,
            device_id={"tp": tp}, device_id_type=MESH)

    def own(j):
        return pltpu.make_async_copy(x.at[pl.ds(j * HALF, HALF)], xs.at[slot["L", j], mine], own_sem.at[j])

    def to_sibling(j):
        return remote(xs.at[slot["L", j], mine], xs.at[slot["L", j], other], sib_send.at[j], sib_recv.at[j], sib)

    def to_far_chip(p):
        j, r, n = PIECES[p]
        rows = pl.ds(r, n)
        return remote(xs.at[slot["L", j], rows], xs.at[slot["R", j], rows], far_send.at[p], far_recv.at[p], far)

    def first():
        return remote(x.at[pl.ds(0, HALF)], xs.at[slot["R", 0], mine], far_send.at[0], far_recv.at[0], far)

    def forward(p):
        i, r, n = PIECES[p]
        s = slot["R", i]
        return remote(xs.at[s, pl.ds(r, n)], xs.at[s, pl.ds(HALF + r, n)], fwd_send.at[p], fwd_recv.at[p], sib)

    moved = pl.ds(HALF + KEPT, MOVED)

    def extra():
        return remote(xs.at[slot["L", LAST], moved], xs.at[slot["R", LAST], moved], extra_sem.at[0], extra_sem.at[1], far)

    def extra_forward():
        s = slot["R", LAST]
        return remote(xs.at[s, moved], xs.at[s, pl.ds(KEPT, MOVED)], extra_sem.at[2], extra_sem.at[3], sib)

    def term_copy(s):
        return remote(to_sib.at[s], from_sib.at[s], term_send.at[s], term_recv.at[s], sib)

    def sum_copy(p):
        i, r, n = PIECES[p]
        rows = pl.ds(i * HALF + r, n)
        return remote(to_far.at[rows], from_far.at[rows], sum_send.at[p], sum_recv.at[p], far)

    def weights(n):
        c = pl.ds(n * NT, NT)
        return (pltpu.make_async_copy(w_gate.at[:, c], wg.at[n], w_sem.at[0, n]),
                pltpu.make_async_copy(w_up.at[:, c], wu.at[n], w_sem.at[1, n]))

    def weights_down(n):
        return pltpu.make_async_copy(w_down.at[:, pl.ds(n * NT, NT)], wd.at[n], w_sem.at[2, n])

    barrier = pltpu.get_barrier_semaphore()
    pl.semaphore_signal(barrier, inc=1, device_id={"tp": far}, device_id_type=MESH)

    @pl.when(core == 1)
    def _():
        pl.semaphore_signal(barrier, inc=1, device_id={"tp": sib}, device_id_type=MESH)

    for j in range(chunks):
        own(j).start()
    pl.semaphore_wait(barrier, 2 - core)
    first().start()

    @pl.when(core == 0)
    def _():
        pl.semaphore_signal(sib_in, inc=1, device_id={"tp": sib}, device_id_type=MESH)

    for j in range(chunks):
        own(j).wait()
        if j:
            to_far_chip(j).start()

    @pl.when(core == 1)
    def _():
        to_far_chip(4).start()

    for n in range(tiles):
        for c in weights(n):
            c.start()

    @pl.when(core == 1)
    def _():
        pl.semaphore_wait(sib_in, 1)

    for j in range(chunks):
        to_sibling(j).start()
    for n in range(dtiles):
        weights_down(n).start()

    def round_term(s):
        def blk(r, _):
            rows = pl.ds(pl.multiple_of(r * BLK, BLK), BLK)
            to_sib[s, rows] = term[lax.rem(s, 2), pl.ds(pl.multiple_of(HALF + r * BLK, BLK), BLK)].astype(BF16)
            return 0
        lax.fori_loop(0, HALF // BLK, blk, 0)

    def chip_sum(s):
        term_copy(s).wait_recv()
        kind, i = ORDER[s]

        def blk(r, _):
            rows = pl.ds(pl.multiple_of(r * BLK, BLK), BLK)
            both = term[s % 2, rows] + from_sib[s, rows].astype(F32)
            at = pl.ds(pl.multiple_of(i * HALF + r * BLK, BLK), BLK)
            if kind == "L":
                local[at] = both
            else:
                to_far[at] = both.astype(BF16)
            return 0
        lax.fori_loop(0, HALF // BLK, blk, 0)

    def start_sum(s):
        kind, i = ORDER[s]
        if kind == "R":
            for p in range(len(PIECES)):
                if PIECES[p][0] == i:
                    sum_copy(p).start()

    def pass_on(i):
        to_far_chip(i).wait_recv()
        forward(i).start()
        if i == LAST:
            @pl.when(core == 1)
            def _():
                to_far_chip(4).wait_recv()
                forward(4).start()
                extra().wait_recv()
                extra_forward().start()

    def step(s, _):
        for k, (kind, i) in enumerate(ORDER):
            @pl.when(s == k)
            def _():
                if kind == "L":
                    if i != LAST:
                        to_sibling(i).wait_recv()
                else:
                    forward(i).wait_recv()
                    if i == LAST:
                        @pl.when(core == 0)
                        def _():
                            forward(4).wait_recv()
                            extra_forward().wait_recv()

        def gate_up(n, _):
            @pl.when(s == 0)
            def _():
                c = pl.ds(0, NT)
                pltpu.make_async_copy(w_gate.at[:, c], wg.at[n], w_sem.at[0, n]).wait()
                pltpu.make_async_copy(w_up.at[:, c], wu.at[n], w_sem.at[1, n]).wait()

            gate = jnp.dot(xs[s], wg[n], preferred_element_type=F32)
            up = jnp.dot(xs[s], wu[n], preferred_element_type=F32)
            hid[:, pl.ds(pl.multiple_of(n * NT, NT), NT)] = (jax.nn.silu(gate) * up).astype(BF16)

            @pl.when((n == 0) & (s > 0))
            def _():
                p = s - 1
                remote(to_sib.at[p], from_sib.at[p], term_send.at[p], term_recv.at[p], sib).start()
            return 0

        lax.fori_loop(0, tiles, gate_up, 0)

        @pl.when(s == 0)
        def _():
            to_sibling(LAST).wait_recv()

            @pl.when(core == 1)
            def _():
                extra().start()

        for k, i in FORWARD_MID.items():
            @pl.when(s == k)
            def _():
                pass_on(i)
        for k in range(1, steps):
            @pl.when(s == k)
            def _():
                chip_sum(k - 1)

        def down(n, _):
            @pl.when(s == 0)
            def _():
                pltpu.make_async_copy(w_down.at[:, pl.ds(0, NT)], wd.at[n], w_sem.at[2, n]).wait()

            cols = pl.ds(pl.multiple_of(n * NT, NT), NT)
            term[lax.rem(s, 2), :, cols] = jnp.dot(hid[...], wd[n], preferred_element_type=F32)
            for k in range(1, steps):
                if ORDER[k - 1][0] == "R":
                    @pl.when((n == 0) & (s == k))
                    def _():
                        start_sum(k - 1)
            return 0

        lax.fori_loop(0, dtiles, down, 0)

        round_term(s)
        for k, i in FORWARD_END.items():
            @pl.when(s == k)
            def _():
                pass_on(i)
        return 0

    lax.fori_loop(0, steps, step, 0)

    def finish(p):
        sum_copy(p).wait_recv()
        i, r, n = PIECES[p]
        rows = pl.ds(i * HALF + r, n)
        out[rows] = (local[rows] + from_far[rows].astype(F32)).astype(BF16)

    last = steps - 1
    finish(0)
    term_copy(last).start()
    chip_sum(last)
    finish(1)
    start_sum(last)
    finish(2)

    for j in range(chunks):
        to_far_chip(j).wait_send()
        to_sibling(j).wait_send()
        forward(j).wait_send()

    @pl.when(core == 1)
    def _():
        to_far_chip(4).wait_send()
        forward(4).wait_send()
        extra().wait_send()
        extra_forward().wait_send()

    for s in range(steps):
        term_copy(s).wait_send()
    for p in range(3):
        sum_copy(p).wait_send()
    for p in range(3, len(PIECES)):
        finish(p)
    for p in range(3, len(PIECES)):
        sum_copy(p).wait_send()


def solution(mesh):
    def step(x, w_gate, w_up, w_down):
        rows, d = x.shape
        f = w_gate.shape[1]
        chunks = rows // HALF
        steps = len(ORDER)
        pieces = len(PIECES)
        dma = pltpu.SemaphoreType.DMA
        return pl.pallas_call(
            kernel,
            out_shape=pltpu.VMEM((rows, d), BF16),
            in_specs=[pl.BlockSpec(memory_space=pl.ANY)] * 4,
            out_specs=pl.BlockSpec(memory_space=pltpu.VMEM),
            scratch_shapes=[
                pltpu.VMEM((steps, M, d), BF16),
                pltpu.VMEM((f // NT, d, NT), BF16),
                pltpu.VMEM((f // NT, d, NT), BF16),
                pltpu.VMEM((d // NT, f, NT), BF16),
                pltpu.VMEM((M, f), BF16),
                pltpu.VMEM((2, M, d), F32),
                pltpu.VMEM((rows, d), F32),
                pltpu.VMEM((steps, HALF, d), BF16),
                pltpu.VMEM((steps, HALF, d), BF16),
                pltpu.VMEM((rows, d), BF16),
                pltpu.VMEM((rows, d), BF16),
                dma((chunks,)),
                dma((3, f // NT)),
                dma((chunks,)), dma((chunks,)),
                dma((pieces,)), dma((pieces,)),
                dma((pieces,)), dma((pieces,)),
                dma((4,)),
                dma((steps,)), dma((steps,)),
                dma((pieces,)), dma((pieces,)),
                pltpu.SemaphoreType.REGULAR,
            ],
            compiler_params=pltpu.CompilerParams(
                collective_id=0, has_side_effects=True, vmem_limit_bytes=63000000),
            name="mlp_ring",
        )(x, w_gate, w_up, w_down)

    return jax.shard_map(
        step,
        mesh=mesh,
        in_specs=(P(("dp", "tp"), None), P(None, "tp"), P(None, "tp"), P("tp", None)),
        out_specs=P(("dp", "tp"), None),
        check_vma=False,
    )
```

```python
import jax
import jax.numpy as jnp
from jax import lax
from jax.experimental import pallas as pl
from jax.experimental.pallas import tpu as pltpu
from jax.sharding import PartitionSpec as P

BF16, F32 = jnp.bfloat16, jnp.float32
MESH = pl.DeviceIdType.MESH

HALF = 128
M = 2 * HALF
NT = 512
BLK = 32
MOVED = 32
KEPT = HALF - MOVED
PIECES = ((0, 0, HALF), (1, 0, HALF), (2, 0, HALF), (3, 0, KEPT), (3, KEPT, MOVED))
LAST = 3

ORDER = (("L", 0), ("L", 1), ("R", 0), ("L", 2), ("R", 1), ("R", 2), ("L", 3), ("R", 3))
SLOT = {k: s for s, k in enumerate(ORDER)}
FORWARD_MID = {1: 0, 4: 2, 5: 3}
FORWARD_END = {2: 1}
LOADS = ((0,), (1,), (2, 3))


def kernel(
    x, w_gate, w_up, w_down, out,
    xs, wgu, wd, hid, term, local, to_sib, from_sib, to_far, from_far,
    load, sib_recv, far_recv, fwd_recv, term_recv, sum_recv, send, sib_in,
):
    me = lax.axis_index("tp")
    core = lax.rem(me, 2)
    sib = me + 1 - 2 * core
    far = lax.rem(me + 2, 4)
    steps = len(ORDER)
    tiles = wd.shape[0]
    chunks = x.shape[0] // HALF
    to_far_sem, to_sib_sem, term_sem = send.at[0], send.at[1], send.at[2]

    def when(c, f):
        pl.when(c)(f)

    def remote(src, dst, send_sem, recv_sem, tp):
        return pltpu.make_async_remote_copy(
            src_ref=src, dst_ref=dst, send_sem=send_sem, recv_sem=recv_sem,
            device_id={"tp": tp}, device_id_type=MESH)

    def arrived(ref, sem):
        remote(ref, ref, sem, sem, far).wait_recv()

    def left(ref, sem):
        remote(ref, ref, sem, sem, far).wait_send()

    def slab(key, first, n):
        return xs.at[pl.ds(SLOT[key] * M + first, n)]

    def own(j):
        return pltpu.make_async_copy(x.at[pl.ds(j * HALF, HALF)], slab(("L", j), 0, HALF), load.at[0])

    def weights(n, sem):
        c = pl.ds(n * NT, NT)
        return (pltpu.make_async_copy(w_gate.at[:, c], wgu.at[2 * n], sem),
                pltpu.make_async_copy(w_up.at[:, c], wgu.at[2 * n + 1], sem))

    def weights_down(n):
        return pltpu.make_async_copy(w_down.at[:, pl.ds(n * NT, NT)], wd.at[n], load.at[len(LOADS)])

    def to_far_chip(p):
        j, r, n = PIECES[p]
        return remote(x.at[pl.ds(j * HALF + r, n)], slab(("R", j), r, n), to_far_sem, far_recv.at[j], far)

    def to_sibling(j):
        return remote(x.at[pl.ds(j * HALF, HALF)], slab(("L", j), HALF, HALF), to_sib_sem, sib_recv.at[min(j, 1)], sib)

    def forward(p):
        i, r, n = PIECES[p]
        return remote(slab(("R", i), r, n), slab(("R", i), HALF + r, n), to_sib_sem, fwd_recv.at[i], sib)

    def extra():
        return remote(slab(("L", LAST), HALF + KEPT, MOVED), slab(("R", LAST), HALF + KEPT, MOVED),
                      to_far_sem, far_recv.at[LAST], far)

    def extra_forward():
        return remote(slab(("R", LAST), HALF + KEPT, MOVED), slab(("R", LAST), KEPT, MOVED),
                      to_sib_sem, fwd_recv.at[LAST], sib)

    def term_copy(s):
        kind, i = ORDER[s]
        return remote(to_sib.at[s], from_sib.at[s], term_sem, term_recv.at[i if kind == "R" else chunks], sib)

    def sum_copy(p):
        i, r, n = PIECES[p]
        rows = pl.ds(i * HALF + r, n)
        return remote(to_far.at[rows], from_far.at[rows], to_far_sem, sum_recv.at[p // LAST_PIECE], far)

    barrier = pltpu.get_barrier_semaphore()
    pl.semaphore_signal(barrier, inc=1, device_id={"tp": far}, device_id_type=MESH)

    @pl.when(core == 1)
    def _():
        pl.semaphore_signal(barrier, inc=1, device_id={"tp": sib}, device_id_type=MESH)

    pl.semaphore_wait(barrier, 2 - core)
    for p in range(LAST_PIECE):
        to_far_chip(p).start()

    @pl.when(core == 0)
    def _():
        pl.semaphore_signal(sib_in, inc=1, device_id={"tp": sib}, device_id_type=MESH)

    @pl.when(core == 1)
    def _():
        to_far_chip(LAST_PIECE).start()

    for j in range(chunks):
        own(j).start()
    for k, group in enumerate(LOADS):
        for n in group:
            for c in weights(n, load.at[k]):
                c.start()

    @pl.when(core == 1)
    def _():
        pl.semaphore_wait(sib_in, 1)

    for j in range(chunks):
        to_sibling(j).start()
    for n in range(tiles):
        weights_down(n).start()

    def pass_on(i):
        if i != LAST:
            arrived(slab(("R", i), 0, HALF), far_recv.at[i])
            forward(i).start()
            return

        @pl.when(core == 0)
        def _():
            arrived(slab(("R", i), 0, KEPT), far_recv.at[i])
            forward(LAST).start()

        @pl.when(core == 1)
        def _():
            arrived(slab(("R", i), 0, HALF + MOVED), far_recv.at[i])
            forward(LAST).start()
            forward(LAST_PIECE).start()
            extra_forward().start()

    def rows_in(k):
        kind, i = ORDER[k]
        if kind == "L":
            if i == 0:
                arrived(slab(("L", 0), HALF, HALF), sib_recv.at[0])
        elif i != LAST:
            arrived(slab(("R", i), HALF, HALF), fwd_recv.at[i])
        else:
            @pl.when(core == 0)
            def _():
                arrived(slab(("R", i), 0, HALF + MOVED), fwd_recv.at[i])

            @pl.when(core == 1)
            def _():
                arrived(slab(("R", i), 0, KEPT), fwd_recv.at[i])

    def blocks(rows, f):
        def blk(r, _):
            f(pl.multiple_of(r * BLK, BLK))
            return 0
        lax.fori_loop(0, rows // BLK, blk, 0)

    def round_term(s):
        def blk(r):
            to_sib[s, pl.ds(r, BLK)] = term[lax.rem(s, 2), pl.ds(pl.multiple_of(HALF + r, BLK), BLK)].astype(BF16)
        blocks(HALF, blk)

    def keep_term(k):
        def blk(r):
            local[pl.ds(pl.multiple_of(ORDER[k][1] * HALF + r, BLK), BLK)] = term[k % 2, pl.ds(r, BLK)]
        blocks(HALF, blk)

    def add_sibling(j):
        def blk(r):
            at = pl.ds(pl.multiple_of(j * HALF + r, BLK), BLK)
            local[at] = local[at] + from_sib[SLOT["L", j], pl.ds(r, BLK)].astype(F32)
        blocks(HALF, blk)

    def chip_sum(k):
        i = ORDER[k][1]
        arrived(from_sib.at[k], term_recv.at[i])

        def blk(r):
            both = term[k % 2, pl.ds(r, BLK)] + from_sib[k, pl.ds(r, BLK)].astype(F32)
            to_far[pl.ds(pl.multiple_of(i * HALF + r, BLK), BLK)] = both.astype(BF16)
        blocks(HALF, blk)

    def start_sum(k):
        for p, (i, _, _) in enumerate(PIECES):
            if i == ORDER[k][1]:
                sum_copy(p).start()

    def step(s, _):
        for k in range(steps):
            when(s == k, lambda: rows_in(k))

        def gate_up(n, _):
            for k, group in enumerate(LOADS):
                count = 2 * len(group) + (1 if k == 0 else 0)
                when((s == 0) & (n == group[0]),
                     lambda: pltpu.make_async_copy(wgu.at[pl.ds(0, count)], wgu.at[pl.ds(0, count)], load.at[k]).wait())

            rows = xs.at[pl.ds(pl.multiple_of(s * M, M), M)]
            gate = jnp.dot(rows[...], wgu[2 * n], preferred_element_type=F32)
            up = jnp.dot(rows[...], wgu[2 * n + 1], preferred_element_type=F32)
            hid[:, pl.ds(pl.multiple_of(n * NT, NT), NT)] = (jax.nn.silu(gate) * up).astype(BF16)

            for k in range(1, steps):
                when((s == k) & (n == 0), lambda: term_copy(k - 1).start())
            return 0

        lax.fori_loop(0, tiles, gate_up, 0)

        @pl.when(s == 0)
        def _():
            pltpu.make_async_copy(wd, wd, load.at[len(LOADS)]).wait()
            arrived(xs.at[pl.ds(0, (chunks - 1) * HALF)], sib_recv.at[1])
            when(core == 1, lambda: extra().start())

        for k, i in FORWARD_MID.items():
            when(s == k, lambda: pass_on(i))
        for k in range(1, steps):
            if ORDER[k - 1][0] == "R":
                when(s == k, lambda: chip_sum(k - 1))

        def down(n, _):
            cols = pl.ds(pl.multiple_of(n * NT, NT), NT)
            term[lax.rem(s, 2), :, cols] = jnp.dot(hid[...], wd[n], preferred_element_type=F32)
            for k in range(1, steps):
                if ORDER[k - 1][0] == "R":
                    when((s == k) & (n == 0), lambda: start_sum(k - 1))
            return 0

        lax.fori_loop(0, tiles, down, 0)

        round_term(s)
        for k in range(steps):
            if ORDER[k][0] == "L":
                when(s == k, lambda: keep_term(k))
        for k, i in FORWARD_END.items():
            when(s == k, lambda: pass_on(i))
        return 0

    lax.fori_loop(0, steps, step, 0)

    last = steps - 1
    arrived(from_sib.at[pl.ds(0, chunks)], term_recv.at[chunks])
    add_sibling(0)
    add_sibling(1)
    term_copy(last).start()
    add_sibling(2)
    chip_sum(last)
    add_sibling(3)
    start_sum(last)

    def finish(p):
        i, r, n = PIECES[p]
        rows = pl.ds(i * HALF + r, n)
        out[rows] = (local[rows] + from_far[rows].astype(F32)).astype(BF16)

    left(to_sib, term_sem)
    sent = x.shape[0] - MOVED, x.shape[0] + MOVED
    for c in range(2):
        when(core == c, lambda: left(xs.at[pl.ds(0, x.shape[0] + sent[c])], to_sib_sem))
    arrived(from_far.at[pl.ds(0, x.shape[0] - MOVED)], sum_recv.at[0])
    for p in range(LAST_PIECE):
        finish(p)
    arrived(from_far.at[pl.ds(0, MOVED)], sum_recv.at[1])
    finish(LAST_PIECE)
    for c in range(2):
        when(core == c, lambda: left(xs.at[pl.ds(0, x.shape[0] + sent[c])], to_far_sem))


LAST_PIECE = len(PIECES) - 1


def solution(mesh):
    def step(x, w_gate, w_up, w_down):
        rows, d = x.shape
        f = w_gate.shape[1]
        chunks = rows // HALF
        steps = len(ORDER)
        dma = pltpu.SemaphoreType.DMA
        return pl.pallas_call(
            kernel,
            out_shape=pltpu.VMEM((rows, d), BF16),
            in_specs=[pl.BlockSpec(memory_space=pl.ANY)] * 4,
            out_specs=pl.BlockSpec(memory_space=pltpu.VMEM),
            scratch_shapes=[
                pltpu.VMEM((steps * M, d), BF16),
                pltpu.VMEM((2 * f // NT, d, NT), BF16),
                pltpu.VMEM((d // NT, f, NT), BF16),
                pltpu.VMEM((M, f), BF16),
                pltpu.VMEM((2, M, d), F32),
                pltpu.VMEM((rows, d), F32),
                pltpu.VMEM((steps, HALF, d), BF16),
                pltpu.VMEM((steps, HALF, d), BF16),
                pltpu.VMEM((rows, d), BF16),
                pltpu.VMEM((rows, d), BF16),
                dma((len(LOADS) + 1,)),
                dma((2,)),
                dma((chunks,)),
                dma((chunks,)),
                dma((chunks + 1,)),
                dma((2,)),
                dma((3,)),
                pltpu.SemaphoreType.REGULAR,
            ],
            compiler_params=pltpu.CompilerParams(
                collective_id=0, has_side_effects=True, vmem_limit_bytes=63000000),
            name="mlp_ring",
        )(x, w_gate, w_up, w_down)

    return jax.shard_map(
        step,
        mesh=mesh,
        in_specs=(P(("dp", "tp"), None), P(None, "tp"), P(None, "tp"), P("tp", None)),
        out_specs=P(("dp", "tp"), None),
        check_vma=False,
    )
```

```python
import jax
import jax.numpy as jnp
from jax import lax
from jax.experimental import pallas as pl
from jax.experimental.pallas import tpu as pltpu
from jax.sharding import PartitionSpec as P

BF16, F32 = jnp.bfloat16, jnp.float32
MESH = pl.DeviceIdType.MESH

HALF = 128
M = 2 * HALF
NT = 512
BLK = 32
MOVED = 32
KEPT = HALF - MOVED
PIECES = ((0, 0, HALF), (1, 0, HALF), (2, 0, HALF), (3, 0, KEPT), (3, KEPT, MOVED))
LAST = 3

ORDER = (("L", 0), ("L", 1), ("R", 0), ("L", 2), ("R", 1), ("R", 2), ("L", 3), ("R", 3))
SLOT = {k: s for s, k in enumerate(ORDER)}
FORWARD_MID = {1: 0, 4: 2, 5: 3}
FORWARD_END = {2: 1}
LOADS = ((0,), (1,), (2, 3))


def kernel(
    x, w_gate, w_up, w_down, out,
    xs, wgu, wd, hid, term, local, to_sib, from_sib, to_far, from_far,
    load, early, far_recv, fwd_recv, own_term, sum_recv, sent, sib_in,
):
    me = lax.axis_index("tp")
    core = lax.rem(me, 2)
    sib = me + 1 - 2 * core
    far = lax.rem(me + 2, 4)
    steps = len(ORDER)
    tiles = wd.shape[0]
    chunks = x.shape[0] // HALF
    depth = x.shape[1]
    sent = sent.at[0]
    sib_recv = (early.at[0], early.at[1])
    fwd_recv = (fwd_recv.at[0], fwd_recv.at[1], early.at[0], early.at[1])
    term_recv = tuple(load.at[i] for i in range(4)) + (own_term.at[0],)

    def when(c, f):
        pl.when(c)(f)

    def remote(src, dst, send_sem, recv_sem, tp):
        return pltpu.make_async_remote_copy(
            src_ref=src, dst_ref=dst, send_sem=send_sem, recv_sem=recv_sem,
            device_id={"tp": tp}, device_id_type=MESH)

    def arrived(ref, sem):
        remote(ref, ref, sem, sem, far).wait_recv()

    def left(ref, sem):
        remote(ref, ref, sem, sem, far).wait_send()

    def slab(key, first, n):
        return xs.at[pl.ds(SLOT[key] * M + first, n)]

    def own(j):
        return pltpu.make_async_copy(x.at[pl.ds(j * HALF, HALF)], slab(("L", j), 0, HALF), load.at[0])

    def weights(n, sem):
        c = pl.ds(n * NT, NT)
        return (pltpu.make_async_copy(w_gate.at[:, c], wgu.at[pl.ds(2 * n * depth, depth)], sem),
                pltpu.make_async_copy(w_up.at[:, c], wgu.at[pl.ds((2 * n + 1) * depth, depth)], sem))

    def weights_down(n):
        return pltpu.make_async_copy(w_down.at[:, pl.ds(n * NT, NT)], wd.at[n], load.at[len(LOADS)])

    def to_far_chip(p):
        j, r, n = PIECES[p]
        return remote(x.at[pl.ds(j * HALF + r, n)], slab(("R", j), r, n), sent, far_recv.at[j], far)

    def to_sibling(j):
        return remote(x.at[pl.ds(j * HALF, HALF)], slab(("L", j), HALF, HALF), sent, sib_recv[min(j, 1)], sib)

    def forward(p):
        i, r, n = PIECES[p]
        return remote(slab(("R", i), r, n), slab(("R", i), HALF + r, n), sent, fwd_recv[i], sib)

    def extra():
        return remote(slab(("L", LAST), HALF + KEPT, MOVED), slab(("R", LAST), HALF + KEPT, MOVED),
                      sent, far_recv.at[LAST], far)

    def extra_forward():
        return remote(slab(("R", LAST), HALF + KEPT, MOVED), slab(("R", LAST), KEPT, MOVED),
                      sent, fwd_recv[LAST], sib)

    def term_copy(s):
        kind, i = ORDER[s]
        return remote(to_sib.at[s], from_sib.at[s], sent, term_recv[i if kind == "R" else chunks], sib)

    def sum_copy(p):
        i, r, n = PIECES[p]
        rows = pl.ds(i * HALF + r, n)
        return remote(to_far.at[rows], from_far.at[rows], sent, sum_recv.at[p // LAST_PIECE], far)

    barrier = pltpu.get_barrier_semaphore()
    pl.semaphore_signal(barrier, inc=1, device_id={"tp": far}, device_id_type=MESH)

    @pl.when(core == 1)
    def _():
        pl.semaphore_signal(barrier, inc=1, device_id={"tp": sib}, device_id_type=MESH)

    pl.semaphore_wait(barrier, 2 - core)
    for p in range(LAST_PIECE):
        to_far_chip(p).start()

    @pl.when(core == 0)
    def _():
        pl.semaphore_signal(sib_in, inc=1, device_id={"tp": sib}, device_id_type=MESH)

    @pl.when(core == 1)
    def _():
        to_far_chip(LAST_PIECE).start()

    for j in range(chunks):
        own(j).start()
    for k, group in enumerate(LOADS):
        for n in group:
            for c in weights(n, load.at[k]):
                c.start()

    @pl.when(core == 1)
    def _():
        pl.semaphore_wait(sib_in, 1)

    for j in range(chunks):
        to_sibling(j).start()
    for n in range(tiles):
        weights_down(n).start()

    def pass_on(i):
        if i != LAST:
            arrived(slab(("R", i), 0, HALF), far_recv.at[i])
            forward(i).start()
            return

        @pl.when(core == 0)
        def _():
            arrived(slab(("R", i), 0, KEPT), far_recv.at[i])
            forward(LAST).start()

        @pl.when(core == 1)
        def _():
            arrived(slab(("R", i), 0, HALF + MOVED), far_recv.at[i])
            forward(LAST).start()
            forward(LAST_PIECE).start()
            extra_forward().start()

    def rows_in(k):
        kind, i = ORDER[k]
        if kind == "L":
            if i == 0:
                arrived(slab(("L", 0), HALF, HALF), sib_recv[0])
        elif i != LAST:
            arrived(slab(("R", i), HALF, HALF), fwd_recv[i])
        else:
            @pl.when(core == 0)
            def _():
                arrived(slab(("R", i), 0, HALF + MOVED), fwd_recv[i])

            @pl.when(core == 1)
            def _():
                arrived(slab(("R", i), 0, KEPT), fwd_recv[i])

    def blocks(rows, f):
        def blk(r, _):
            f(pl.multiple_of(r * BLK, BLK))
            return 0
        lax.fori_loop(0, rows // BLK, blk, 0)

    def round_term(s):
        def blk(r):
            to_sib[s, pl.ds(r, BLK)] = term[lax.rem(s, 2), pl.ds(pl.multiple_of(HALF + r, BLK), BLK)].astype(BF16)
        blocks(HALF, blk)

    def keep_term(k):
        def blk(r):
            local[pl.ds(pl.multiple_of(ORDER[k][1] * HALF + r, BLK), BLK)] = term[k % 2, pl.ds(r, BLK)]
        blocks(HALF, blk)

    def add_sibling(j):
        def blk(r):
            at = pl.ds(pl.multiple_of(j * HALF + r, BLK), BLK)
            local[at] = local[at] + from_sib[SLOT["L", j], pl.ds(r, BLK)].astype(F32)
        blocks(HALF, blk)

    def chip_sum(k):
        i = ORDER[k][1]
        arrived(from_sib.at[k], term_recv[i])

        def blk(r):
            both = term[k % 2, pl.ds(r, BLK)] + from_sib[k, pl.ds(r, BLK)].astype(F32)
            to_far[pl.ds(pl.multiple_of(i * HALF + r, BLK), BLK)] = both.astype(BF16)
        blocks(HALF, blk)

    def start_sum(k):
        for p, (i, _, _) in enumerate(PIECES):
            if i == ORDER[k][1]:
                sum_copy(p).start()

    def step(s, _):
        for k in range(steps):
            when(s == k, lambda: rows_in(k))

        def gate_up(n, _):
            for k, group in enumerate(LOADS):
                count = 2 * len(group) + (1 if k == 0 else 0)
                when((s == 0) & (n == group[0]),
                     lambda: pltpu.make_async_copy(
                         wgu.at[pl.ds(0, count * depth)], wgu.at[pl.ds(0, count * depth)], load.at[k]).wait())

            rows = xs.at[pl.ds(pl.multiple_of(s * M, M), M)]
            w = pl.multiple_of(2 * n * depth, depth)
            gate = jnp.dot(rows[...], wgu[pl.ds(w, depth)], preferred_element_type=F32)
            up = jnp.dot(rows[...], wgu[pl.ds(pl.multiple_of(w + depth, depth), depth)], preferred_element_type=F32)
            hid[:, pl.ds(pl.multiple_of(n * NT, NT), NT)] = (jax.nn.silu(gate) * up).astype(BF16)

            for k in range(1, steps):
                when((s == k) & (n == 0), lambda: term_copy(k - 1).start())
            return 0

        lax.fori_loop(0, tiles, gate_up, 0)

        @pl.when(s == 0)
        def _():
            pltpu.make_async_copy(wd, wd, load.at[len(LOADS)]).wait()
            arrived(xs.at[pl.ds(0, (chunks - 1) * HALF)], sib_recv[1])
            when(core == 1, lambda: extra().start())

        for k in range(1, steps):
            if ORDER[k - 1][0] == "R":
                when(s == k, lambda: chip_sum(k - 1))
        for k, i in FORWARD_MID.items():
            when(s == k, lambda: pass_on(i))

        def down(n, _):
            cols = pl.ds(pl.multiple_of(n * NT, NT), NT)
            term[lax.rem(s, 2), :, cols] = jnp.dot(hid[...], wd[n], preferred_element_type=F32)
            for k in range(1, steps):
                if ORDER[k - 1][0] == "R":
                    when((s == k) & (n == 0), lambda: start_sum(k - 1))
            return 0

        lax.fori_loop(0, tiles, down, 0)

        round_term(s)
        for k in range(steps):
            if ORDER[k][0] == "L":
                when(s == k, lambda: keep_term(k))
        for k, i in FORWARD_END.items():
            when(s == k, lambda: pass_on(i))
        return 0

    lax.fori_loop(0, steps, step, 0)

    last = steps - 1
    arrived(from_sib.at[pl.ds(0, chunks)], term_recv[chunks])
    add_sibling(0)
    add_sibling(1)
    term_copy(last).start()
    add_sibling(2)
    chip_sum(last)
    add_sibling(3)
    start_sum(last)

    def finish(p):
        i, r, n = PIECES[p]
        rows = pl.ds(i * HALF + r, n)
        out[rows] = (local[rows] + from_far[rows].astype(F32)).astype(BF16)

    arrived(from_far.at[pl.ds(0, x.shape[0] - MOVED)], sum_recv.at[0])
    for p in range(LAST_PIECE):
        finish(p)
    arrived(from_far.at[pl.ds(0, MOVED)], sum_recv.at[1])
    finish(LAST_PIECE)
    rows = x.shape[0]
    for c, far_rows in enumerate((rows - MOVED, rows + MOVED)):
        total = 2 * (far_rows + rows) + steps * HALF
        when(core == c, lambda: left(wgu.at[pl.ds(0, total * x.shape[1] // NT)], sent))


LAST_PIECE = len(PIECES) - 1


def solution(mesh):
    def step(x, w_gate, w_up, w_down):
        rows, d = x.shape
        f = w_gate.shape[1]
        chunks = rows // HALF
        steps = len(ORDER)
        dma = pltpu.SemaphoreType.DMA
        return pl.pallas_call(
            kernel,
            out_shape=pltpu.VMEM((rows, d), BF16),
            in_specs=[pl.BlockSpec(memory_space=pl.ANY)] * 4,
            out_specs=pl.BlockSpec(memory_space=pltpu.VMEM),
            scratch_shapes=[
                pltpu.VMEM((steps * M, d), BF16),
                pltpu.VMEM((2 * f // NT * d, NT), BF16),
                pltpu.VMEM((d // NT, f, NT), BF16),
                pltpu.VMEM((M, f), BF16),
                pltpu.VMEM((2, M, d), F32),
                pltpu.VMEM((rows, d), F32),
                pltpu.VMEM((steps, HALF, d), BF16),
                pltpu.VMEM((steps, HALF, d), BF16),
                pltpu.VMEM((rows, d), BF16),
                pltpu.VMEM((rows, d), BF16),
                dma((len(LOADS) + 1,)),
                dma((2,)),
                dma((chunks,)),
                dma((2,)),
                dma((1,)),
                dma((2,)),
                dma((1,)),
                pltpu.SemaphoreType.REGULAR,
            ],
            compiler_params=pltpu.CompilerParams(
                collective_id=0, has_side_effects=True, vmem_limit_bytes=63000000),
            name="mlp_ring",
        )(x, w_gate, w_up, w_down)

    return jax.shard_map(
        step,
        mesh=mesh,
        in_specs=(P(("dp", "tp"), None), P(None, "tp"), P(None, "tp"), P("tp", None)),
        out_specs=P(("dp", "tp"), None),
        check_vma=False,
    )
```

```python
import jax
import jax.numpy as jnp
from jax import lax
from jax.experimental import pallas as pl
from jax.experimental.pallas import tpu as pltpu
from jax.sharding import PartitionSpec as P

BF16, F32 = jnp.bfloat16, jnp.float32
MESH = pl.DeviceIdType.MESH

HALF = 128
M = 2 * HALF
NT = 1024
BLK = 32
MOVED = 32
KEPT = HALF - MOVED
PIECES = ((0, 0, HALF), (1, 0, HALF), (2, 0, HALF), (3, 0, KEPT), (3, KEPT, MOVED))
LAST = 3

ORDER = (("L", 0), ("L", 1), ("R", 0), ("L", 2), ("R", 1), ("R", 2), ("L", 3), ("R", 3))
SLOT = {k: s for s, k in enumerate(ORDER)}
FORWARD_MID = {1: 0, 4: 2, 5: 3}
FORWARD_END = {2: 1}


def kernel(
    x, w_gate, w_up, w_down, out,
    xs, wgu, wd, hid, term, local, to_sib, from_sib, to_far, from_far,
    load, early, far_recv, fwd_recv, own_term, sum_recv, sent, sib_in,
):
    me = lax.axis_index("tp")
    core = lax.rem(me, 2)
    sib = me + 1 - 2 * core
    far = lax.rem(me + 2, 4)
    steps = len(ORDER)
    tiles = wd.shape[0]
    chunks = x.shape[0] // HALF
    depth = x.shape[1]
    sent = sent.at[0]
    sib_recv = (early.at[0], early.at[1])
    fwd_recv = (fwd_recv.at[0], fwd_recv.at[1], early.at[0], early.at[1])
    term_recv = tuple(far_recv.at[i] for i in range(4)) + (own_term.at[0],)

    def when(c, f):
        pl.when(c)(f)

    def remote(src, dst, send_sem, recv_sem, tp):
        return pltpu.make_async_remote_copy(
            src_ref=src, dst_ref=dst, send_sem=send_sem, recv_sem=recv_sem,
            device_id={"tp": tp}, device_id_type=MESH)

    def arrived(ref, sem):
        remote(ref, ref, sem, sem, far).wait_recv()

    def left(ref, sem):
        remote(ref, ref, sem, sem, far).wait_send()

    def slab(key, first, n):
        return xs.at[pl.ds(SLOT[key] * M + first, n)]

    def own(j):
        return pltpu.make_async_copy(x.at[pl.ds(j * HALF, HALF)], slab(("L", j), 0, HALF), sib_recv[0])

    def weights(n):
        c = pl.ds(n * NT, NT)
        return (pltpu.make_async_copy(w_gate.at[:, c], wgu.at[pl.ds(2 * n * depth, depth)], load.at[0]),
                pltpu.make_async_copy(w_up.at[:, c], wgu.at[pl.ds((2 * n + 1) * depth, depth)], load.at[0]))

    def weights_down(n):
        return pltpu.make_async_copy(w_down.at[:, pl.ds(n * NT, NT)], wd.at[n], load.at[1])

    def to_far_chip(p):
        j, r, n = PIECES[p]
        return remote(x.at[pl.ds(j * HALF + r, n)], slab(("R", j), r, n), sent, far_recv.at[j], far)

    def to_sibling(j):
        return remote(x.at[pl.ds(j * HALF, HALF)], slab(("L", j), HALF, HALF), sent, sib_recv[min(j, 1)], sib)

    def forward(p):
        i, r, n = PIECES[p]
        return remote(slab(("R", i), r, n), slab(("R", i), HALF + r, n), sent, fwd_recv[i], sib)

    def extra():
        return remote(slab(("L", LAST), HALF + KEPT, MOVED), slab(("R", LAST), HALF + KEPT, MOVED),
                      sent, far_recv.at[LAST], far)

    def extra_forward():
        return remote(slab(("R", LAST), HALF + KEPT, MOVED), slab(("R", LAST), KEPT, MOVED),
                      sent, fwd_recv[LAST], sib)

    def term_copy(s):
        kind, i = ORDER[s]
        return remote(to_sib.at[s], from_sib.at[s], sent, term_recv[i if kind == "R" else chunks], sib)

    def sum_copy(p):
        i, r, n = PIECES[p]
        rows = pl.ds(i * HALF + r, n)
        return remote(to_far.at[rows], from_far.at[rows], sent, sum_recv.at[p // LAST_PIECE], far)

    barrier = pltpu.get_barrier_semaphore()
    pl.semaphore_signal(barrier, inc=1, device_id={"tp": far}, device_id_type=MESH)

    @pl.when(core == 1)
    def _():
        pl.semaphore_signal(barrier, inc=1, device_id={"tp": sib}, device_id_type=MESH)

    pl.semaphore_wait(barrier, 2 - core)
    for p in range(LAST_PIECE):
        to_far_chip(p).start()

    @pl.when(core == 0)
    def _():
        pl.semaphore_signal(sib_in, inc=1, device_id={"tp": sib}, device_id_type=MESH)

    @pl.when(core == 1)
    def _():
        to_far_chip(LAST_PIECE).start()

    for j in range(chunks):
        own(j).start()
    for n in range(tiles):
        for c in weights(n):
            c.start()

    @pl.when(core == 1)
    def _():
        pl.semaphore_wait(sib_in, 1)

    for j in range(chunks):
        to_sibling(j).start()
    for n in range(tiles):
        weights_down(n).start()

    def pass_on(i):
        if i != LAST:
            arrived(slab(("R", i), 0, HALF), far_recv.at[i])
            forward(i).start()
            return

        @pl.when(core == 0)
        def _():
            arrived(slab(("R", i), 0, KEPT), far_recv.at[i])
            forward(LAST).start()

        @pl.when(core == 1)
        def _():
            arrived(slab(("R", i), 0, HALF + MOVED), far_recv.at[i])
            forward(LAST).start()
            forward(LAST_PIECE).start()
            extra_forward().start()

    def rows_in(k):
        kind, i = ORDER[k]
        if kind == "L":
            if i == 0:
                arrived(xs.at[pl.ds(0, x.shape[0] + HALF)], sib_recv[0])
                arrived(wgu, load.at[0])
        elif i != LAST:
            arrived(slab(("R", i), HALF, HALF), fwd_recv[i])
        else:
            @pl.when(core == 0)
            def _():
                arrived(slab(("R", i), 0, HALF + MOVED), fwd_recv[i])

            @pl.when(core == 1)
            def _():
                arrived(slab(("R", i), 0, KEPT), fwd_recv[i])

    def blocks(rows, f):
        def blk(r, _):
            f(pl.multiple_of(r * BLK, BLK))
            return 0
        lax.fori_loop(0, rows // BLK, blk, 0)

    def round_term(s):
        def blk(r):
            to_sib[s, pl.ds(r, BLK)] = term[lax.rem(s, 2), pl.ds(pl.multiple_of(HALF + r, BLK), BLK)].astype(BF16)
        blocks(HALF, blk)

    def keep_term(k):
        def blk(r):
            local[pl.ds(pl.multiple_of(ORDER[k][1] * HALF + r, BLK), BLK)] = term[k % 2, pl.ds(r, BLK)]
        blocks(HALF, blk)

    def add_sibling(j):
        def blk(r):
            at = pl.ds(pl.multiple_of(j * HALF + r, BLK), BLK)
            local[at] = local[at] + from_sib[SLOT["L", j], pl.ds(r, BLK)].astype(F32)
        blocks(HALF, blk)

    def chip_sum(k):
        i = ORDER[k][1]
        arrived(from_sib.at[k], term_recv[i])

        def blk(r):
            both = term[k % 2, pl.ds(r, BLK)] + from_sib[k, pl.ds(r, BLK)].astype(F32)
            to_far[pl.ds(pl.multiple_of(i * HALF + r, BLK), BLK)] = both.astype(BF16)
        blocks(HALF, blk)

    def start_sum(k):
        for p, (i, _, _) in enumerate(PIECES):
            if i == ORDER[k][1]:
                sum_copy(p).start()

    def step(s, _):
        for k in range(steps):
            when(s == k, lambda: rows_in(k))

        def gate_up(n, _):
            rows = xs.at[pl.ds(pl.multiple_of(s * M, M), M)]
            w = pl.multiple_of(2 * n * depth, depth)
            gate = jnp.dot(rows[...], wgu[pl.ds(w, depth)], preferred_element_type=F32)
            up = jnp.dot(rows[...], wgu[pl.ds(pl.multiple_of(w + depth, depth), depth)], preferred_element_type=F32)
            hid[:, pl.ds(pl.multiple_of(n * NT, NT), NT)] = (jax.nn.silu(gate) * up).astype(BF16)

            for k in range(1, steps):
                when((s == k) & (n == 0), lambda: term_copy(k - 1).start())
            return 0

        lax.fori_loop(0, tiles, gate_up, 0)

        @pl.when(s == 0)
        def _():
            arrived(wd, load.at[1])
            arrived(xs.at[pl.ds(0, (chunks - 1) * HALF)], sib_recv[1])
            when(core == 1, lambda: extra().start())

        for k in range(1, steps):
            if ORDER[k - 1][0] == "R":
                when(s == k, lambda: chip_sum(k - 1))
        for k, i in FORWARD_MID.items():
            when(s == k, lambda: pass_on(i))

        def down(n, _):
            cols = pl.ds(pl.multiple_of(n * NT, NT), NT)
            term[lax.rem(s, 2), :, cols] = jnp.dot(hid[...], wd[n], preferred_element_type=F32)
            for k in range(1, steps):
                if ORDER[k - 1][0] == "R":
                    when((s == k) & (n == 0), lambda: start_sum(k - 1))
            return 0

        lax.fori_loop(0, tiles, down, 0)

        round_term(s)
        for k in range(steps):
            if ORDER[k][0] == "L":
                when(s == k, lambda: keep_term(k))
        for k, i in FORWARD_END.items():
            when(s == k, lambda: pass_on(i))
        return 0

    lax.fori_loop(0, steps, step, 0)

    last = steps - 1
    arrived(from_sib.at[pl.ds(0, chunks)], term_recv[chunks])
    add_sibling(0)
    add_sibling(1)
    term_copy(last).start()
    add_sibling(2)
    chip_sum(last)
    add_sibling(3)
    start_sum(last)

    def finish(p):
        i, r, n = PIECES[p]
        rows = pl.ds(i * HALF + r, n)
        out[rows] = (local[rows] + from_far[rows].astype(F32)).astype(BF16)

    arrived(from_far.at[pl.ds(0, x.shape[0] - MOVED)], sum_recv.at[0])
    for p in range(LAST_PIECE):
        finish(p)
    arrived(from_far.at[pl.ds(0, MOVED)], sum_recv.at[1])
    finish(LAST_PIECE)
    rows = x.shape[0]
    for c, far_rows in enumerate((rows - MOVED, rows + MOVED)):
        total = 2 * (far_rows + rows) + steps * HALF
        when(core == c, lambda: left(wgu.at[pl.ds(0, total * x.shape[1] // NT)], sent))


LAST_PIECE = len(PIECES) - 1


def solution(mesh):
    def step(x, w_gate, w_up, w_down):
        rows, d = x.shape
        f = w_gate.shape[1]
        chunks = rows // HALF
        steps = len(ORDER)
        dma = pltpu.SemaphoreType.DMA
        return pl.pallas_call(
            kernel,
            out_shape=pltpu.VMEM((rows, d), BF16),
            in_specs=[pl.BlockSpec(memory_space=pl.ANY)] * 4,
            out_specs=pl.BlockSpec(memory_space=pltpu.VMEM),
            scratch_shapes=[
                pltpu.VMEM((steps * M, d), BF16),
                pltpu.VMEM((2 * f // NT * d, NT), BF16),
                pltpu.VMEM((d // NT, f, NT), BF16),
                pltpu.VMEM((M, f), BF16),
                pltpu.VMEM((2, M, d), F32),
                pltpu.VMEM((rows, d), F32),
                pltpu.VMEM((steps, HALF, d), BF16),
                pltpu.VMEM((steps, HALF, d), BF16),
                pltpu.VMEM((rows, d), BF16),
                pltpu.VMEM((rows, d), BF16),
                dma((2,)),
                dma((2,)),
                dma((chunks,)),
                dma((2,)),
                dma((1,)),
                dma((2,)),
                dma((1,)),
                pltpu.SemaphoreType.REGULAR,
            ],
            compiler_params=pltpu.CompilerParams(
                collective_id=0, has_side_effects=True, vmem_limit_bytes=63000000),
            name="mlp_ring",
        )(x, w_gate, w_up, w_down)

    return jax.shard_map(
        step,
        mesh=mesh,
        in_specs=(P(("dp", "tp"), None), P(None, "tp"), P(None, "tp"), P("tp", None)),
        out_specs=P(("dp", "tp"), None),
        check_vma=False,
    )
```

```python
import jax
import jax.numpy as jnp
from jax import lax
from jax.experimental import pallas as pl
from jax.experimental.pallas import tpu as pltpu
from jax.sharding import PartitionSpec as P

BF16, F32 = jnp.bfloat16, jnp.float32
MESH = pl.DeviceIdType.MESH

HALF = 128
M = 2 * HALF
NT = 1024
BLK = 32
MOVED = 48
KEPT = HALF - MOVED
PIECES = ((0, 0, HALF), (1, 0, HALF), (2, 0, HALF), (3, 0, KEPT), (3, KEPT, MOVED))
LAST = 3
ROUND = (16, 768)

ORDER = (("L", 0), ("L", 1), ("R", 0), ("L", 2), ("R", 1), ("R", 2), ("L", 3), ("R", 3))
SLOT = {k: s for s, k in enumerate(ORDER)}
FORWARD_MID = {1: 0, 4: 2, 5: 3}
FORWARD_END = {2: 1}


def kernel(
    x, w_gate, w_up, w_down, out,
    xs, wgu, wd, hid, term, local, to_sib, from_sib, to_far, from_far,
    load, early, far_recv, fwd_recv, own_term, sum_recv, sent, sib_in, relay, relay_sem,
):
    me = lax.axis_index("tp")
    core = lax.rem(me, 2)
    sib = me + 1 - 2 * core
    far = lax.rem(me + 2, 4)
    dp, chip = lax.axis_index("dp"), lax.div(me, 2)
    giver = (core == 0) & (dp == 0) & (chip == 1)
    first_hop = (core == 0) & (dp == 1) & (chip == 1)
    second_hop = (core == 0) & (dp == 1) & (chip == 0)
    across = dp + chip - 2 * dp * chip
    steps = len(ORDER)
    tiles = wd.shape[0]
    chunks = x.shape[0] // HALF
    depth = x.shape[1]
    sent = sent.at[0]
    sib_recv = (early.at[0], early.at[1])
    fwd_recv = (fwd_recv.at[0], fwd_recv.at[1], early.at[0], early.at[1])
    term_recv = tuple(far_recv.at[i] for i in range(4)) + (own_term.at[0],)

    def when(c, f):
        pl.when(c)(f)

    def remote(src, dst, send_sem, recv_sem, tp):
        return pltpu.make_async_remote_copy(
            src_ref=src, dst_ref=dst, send_sem=send_sem, recv_sem=recv_sem,
            device_id={"tp": tp}, device_id_type=MESH)

    def arrived(ref, sem):
        remote(ref, ref, sem, sem, far).wait_recv()

    def left(ref, sem):
        remote(ref, ref, sem, sem, far).wait_send()

    def slab(key, first, n):
        return xs.at[pl.ds(SLOT[key] * M + first, n)]

    def own(j):
        return pltpu.make_async_copy(x.at[pl.ds(j * HALF, HALF)], slab(("L", j), 0, HALF), sib_recv[0])

    def weights(n):
        c = pl.ds(n * NT, NT)
        return (pltpu.make_async_copy(w_gate.at[:, c], wgu.at[pl.ds(2 * n * depth, depth)], load.at[0]),
                pltpu.make_async_copy(w_up.at[:, c], wgu.at[pl.ds((2 * n + 1) * depth, depth)], load.at[0]))

    def weights_down(n):
        return pltpu.make_async_copy(w_down.at[:, pl.ds(n * NT, NT)], wd.at[n], load.at[1])

    def to_far_chip(p):
        j, r, n = PIECES[p]
        return remote(x.at[pl.ds(j * HALF + r, n)], slab(("R", j), r, n), sent, far_recv.at[j], far)

    def to_sibling(j):
        return remote(x.at[pl.ds(j * HALF, HALF)], slab(("L", j), HALF, HALF), sent, sib_recv[min(j, 1)], sib)

    def forward(p):
        i, r, n = PIECES[p]
        return remote(slab(("R", i), r, n), slab(("R", i), HALF + r, n), sent, fwd_recv[i], sib)

    def extra():
        return remote(slab(("L", LAST), HALF + KEPT, MOVED), slab(("R", LAST), HALF + KEPT, MOVED),
                      sent, far_recv.at[LAST], far)

    def extra_forward():
        return remote(slab(("R", LAST), HALF + KEPT, MOVED), slab(("R", LAST), KEPT, MOVED),
                      sent, fwd_recv[LAST], sib)

    round_rows = KEPT - ROUND[0]

    def over_y(src, dst, send_sem, recv_sem):
        return pltpu.make_async_remote_copy(
            src_ref=src, dst_ref=dst, send_sem=send_sem, recv_sem=recv_sem,
            device_id={"dp": 1 - dp}, device_id_type=MESH)

    def give():
        src = x.at[pl.ds(LAST * HALF + round_rows, ROUND[0]), pl.ds(0, ROUND[1])]
        return over_y(src, relay.at[0], sent, relay_sem.at[0])

    def relay_on():
        return remote(relay.at[0], relay.at[1], load.at[0], relay_sem.at[0], far)

    def hand_over():
        dst = xs.at[pl.ds(SLOT["R", LAST] * M + round_rows, ROUND[0]), pl.ds(0, ROUND[1])]
        return over_y(relay.at[1], dst, load.at[0], far_recv.at[LAST])

    def not_given():
        at, to = LAST * HALF, SLOT["R", LAST] * M
        rest = pl.ds(ROUND[1], depth - ROUND[1])
        return (remote(x.at[pl.ds(at, round_rows)], xs.at[pl.ds(to, round_rows)], sent, far_recv.at[LAST], far),
                remote(x.at[pl.ds(at + round_rows, ROUND[0]), rest],
                       xs.at[pl.ds(to + round_rows, ROUND[0]), rest], sent, far_recv.at[LAST], far))

    def term_copy(s):
        kind, i = ORDER[s]
        return remote(to_sib.at[s], from_sib.at[s], sent, term_recv[i if kind == "R" else chunks], sib)

    def sum_copy(p):
        i, r, n = PIECES[p]
        rows = pl.ds(i * HALF + r, n)
        return remote(to_far.at[rows], from_far.at[rows], sent, sum_recv.at[p // LAST_PIECE], far)

    barrier = pltpu.get_barrier_semaphore()
    pl.semaphore_signal(barrier, inc=1, device_id={"tp": far}, device_id_type=MESH)

    @pl.when(core == 1)
    def _():
        pl.semaphore_signal(barrier, inc=1, device_id={"tp": sib}, device_id_type=MESH)

    @pl.when((core == 0) & (across == 0))
    def _():
        pl.semaphore_signal(barrier, inc=1, device_id={"dp": 1 - dp}, device_id_type=MESH)

    pl.semaphore_wait(barrier, 2 - core + (1 - core) * across)
    for p in range(2):
        to_far_chip(p).start()
    when(giver, lambda: give().start())

    @pl.when(core == 0)
    def _():
        pl.semaphore_signal(sib_in, inc=1, device_id={"tp": sib}, device_id_type=MESH)

    for j in range(chunks):
        own(j).start()
    for n in range(tiles):
        for c in weights(n):
            c.start()

    @pl.when(core == 1)
    def _():
        pl.semaphore_wait(sib_in, 1)

    for j in range(chunks):
        to_sibling(j).start()
    for n in range(tiles):
        weights_down(n).start()

    def pass_on(i):
        if i != LAST:
            arrived(slab(("R", i), 0, HALF), far_recv.at[i])
            forward(i).start()
            return

        @pl.when(core == 0)
        def _():
            arrived(slab(("R", i), 0, KEPT), far_recv.at[i])
            forward(LAST).start()

        @pl.when(core == 1)
        def _():
            arrived(slab(("R", i), 0, HALF + MOVED), far_recv.at[i])
            forward(LAST).start()
            forward(LAST_PIECE).start()
            extra_forward().start()

    def rows_in(k):
        kind, i = ORDER[k]
        if kind == "L":
            if i == 0:
                arrived(xs.at[pl.ds(0, x.shape[0] + HALF)], sib_recv[0])
                arrived(wgu, load.at[0])
        elif i != LAST:
            arrived(slab(("R", i), HALF, HALF), fwd_recv[i])
        else:
            @pl.when(core == 0)
            def _():
                arrived(slab(("R", i), 0, HALF + MOVED), fwd_recv[i])

            @pl.when(core == 1)
            def _():
                arrived(slab(("R", i), 0, KEPT), fwd_recv[i])

    def blocks(rows, f):
        def blk(r, _):
            f(pl.multiple_of(r * BLK, BLK))
            return 0
        lax.fori_loop(0, rows // BLK, blk, 0)

    def round_term(s):
        def blk(r):
            to_sib[s, pl.ds(r, BLK)] = term[lax.rem(s, 2), pl.ds(pl.multiple_of(HALF + r, BLK), BLK)].astype(BF16)
        blocks(HALF, blk)

    def keep_term(k):
        def blk(r):
            local[pl.ds(pl.multiple_of(ORDER[k][1] * HALF + r, BLK), BLK)] = term[k % 2, pl.ds(r, BLK)]
        blocks(HALF, blk)

    def add_sibling(j):
        def blk(r):
            at = pl.ds(pl.multiple_of(j * HALF + r, BLK), BLK)
            local[at] = local[at] + from_sib[SLOT["L", j], pl.ds(r, BLK)].astype(F32)
        blocks(HALF, blk)

    def chip_sum(k):
        i = ORDER[k][1]
        arrived(from_sib.at[k], term_recv[i])

        def blk(r):
            both = term[k % 2, pl.ds(r, BLK)] + from_sib[k, pl.ds(r, BLK)].astype(F32)
            to_far[pl.ds(pl.multiple_of(i * HALF + r, BLK), BLK)] = both.astype(BF16)
        blocks(HALF, blk)

    def start_sum(k):
        for p, (i, _, _) in enumerate(PIECES):
            if i == ORDER[k][1]:
                sum_copy(p).start()

    def step(s, _):
        for k in range(steps):
            when(s == k, lambda: rows_in(k))

        def gate_up(n, _):
            rows = xs.at[pl.ds(pl.multiple_of(s * M, M), M)]
            w = pl.multiple_of(2 * n * depth, depth)
            gate = jnp.dot(rows[...], wgu[pl.ds(w, depth)], preferred_element_type=F32)
            up = jnp.dot(rows[...], wgu[pl.ds(pl.multiple_of(w + depth, depth), depth)], preferred_element_type=F32)
            hid[:, pl.ds(pl.multiple_of(n * NT, NT), NT)] = (jax.nn.silu(gate) * up).astype(BF16)

            for k in range(1, steps):
                when((s == k) & (n == 0), lambda: term_copy(k - 1).start())
            return 0

        lax.fori_loop(0, tiles, gate_up, 0)

        @pl.when(s == 0)
        def _():
            arrived(wd, load.at[1])
            arrived(xs.at[pl.ds(0, (chunks - 1) * HALF)], sib_recv[1])

            @pl.when(first_hop)
            def _():
                arrived(relay.at[0], relay_sem.at[0])
                relay_on().start()

            to_far_chip(2).start()

            @pl.when(giver)
            def _():
                for c in not_given():
                    c.start()

            @pl.when(jnp.logical_not(giver))
            def _():
                to_far_chip(LAST).start()

            @pl.when(core == 1)
            def _():
                to_far_chip(LAST_PIECE).start()
                extra().start()

        @pl.when((s == 3) & second_hop)
        def _():
            arrived(relay.at[1], relay_sem.at[0])
            hand_over().start()

        for k in range(1, steps):
            if ORDER[k - 1][0] == "R":
                when(s == k, lambda: chip_sum(k - 1))
        for k, i in FORWARD_MID.items():
            when(s == k, lambda: pass_on(i))

        def down(n, _):
            cols = pl.ds(pl.multiple_of(n * NT, NT), NT)
            term[lax.rem(s, 2), :, cols] = jnp.dot(hid[...], wd[n], preferred_element_type=F32)
            for k in range(1, steps):
                if ORDER[k - 1][0] == "R":
                    when((s == k) & (n == 0), lambda: start_sum(k - 1))
            return 0

        lax.fori_loop(0, tiles, down, 0)

        round_term(s)
        for k in range(steps):
            if ORDER[k][0] == "L":
                when(s == k, lambda: keep_term(k))
        for k, i in FORWARD_END.items():
            when(s == k, lambda: pass_on(i))
        return 0

    lax.fori_loop(0, steps, step, 0)

    last = steps - 1
    arrived(from_sib.at[pl.ds(0, chunks)], term_recv[chunks])
    add_sibling(0)
    add_sibling(1)
    term_copy(last).start()
    add_sibling(2)
    chip_sum(last)
    add_sibling(3)
    start_sum(last)

    def finish(p):
        i, r, n = PIECES[p]
        rows = pl.ds(i * HALF + r, n)
        out[rows] = (local[rows] + from_far[rows].astype(F32)).astype(BF16)

    when(first_hop | second_hop, lambda: left(relay.at[0], load.at[0]))
    arrived(from_far.at[pl.ds(0, x.shape[0] - MOVED)], sum_recv.at[0])
    for p in range(LAST_PIECE):
        finish(p)
    arrived(from_far.at[pl.ds(0, MOVED)], sum_recv.at[1])
    finish(LAST_PIECE)
    rows = x.shape[0]
    for c, far_rows in enumerate((rows - MOVED, rows + MOVED)):
        total = 2 * (far_rows + rows) + steps * HALF
        when(core == c, lambda: left(wgu.at[pl.ds(0, total * depth // NT)], sent))


LAST_PIECE = len(PIECES) - 1


def solution(mesh):
    def step(x, w_gate, w_up, w_down):
        rows, d = x.shape
        f = w_gate.shape[1]
        chunks = rows // HALF
        steps = len(ORDER)
        dma = pltpu.SemaphoreType.DMA
        return pl.pallas_call(
            kernel,
            out_shape=pltpu.VMEM((rows, d), BF16),
            in_specs=[pl.BlockSpec(memory_space=pl.ANY)] * 4,
            out_specs=pl.BlockSpec(memory_space=pltpu.VMEM),
            scratch_shapes=[
                pltpu.VMEM((steps * M, d), BF16),
                pltpu.VMEM((2 * f // NT * d, NT), BF16),
                pltpu.VMEM((d // NT, f, NT), BF16),
                pltpu.VMEM((M, f), BF16),
                pltpu.VMEM((2, M, d), F32),
                pltpu.VMEM((rows, d), F32),
                pltpu.VMEM((steps, HALF, d), BF16),
                pltpu.VMEM((steps, HALF, d), BF16),
                pltpu.VMEM((rows, d), BF16),
                pltpu.VMEM((rows, d), BF16),
                dma((2,)),
                dma((2,)),
                dma((chunks,)),
                dma((2,)),
                dma((1,)),
                dma((2,)),
                dma((1,)),
                pltpu.SemaphoreType.REGULAR,
                pltpu.VMEM((2, *ROUND), BF16),
                dma((1,)),
            ],
            compiler_params=pltpu.CompilerParams(
                collective_id=0, has_side_effects=True, vmem_limit_bytes=63000000),
            name="mlp_ring",
        )(x, w_gate, w_up, w_down)

    return jax.shard_map(
        step,
        mesh=mesh,
        in_specs=(P(("dp", "tp"), None), P(None, "tp"), P(None, "tp"), P("tp", None)),
        out_specs=P(("dp", "tp"), None),
        check_vma=False,
    )
```

```python
import jax
import jax.numpy as jnp
from jax import lax
from jax.experimental import pallas as pl
from jax.experimental.pallas import tpu as pltpu
from jax.sharding import PartitionSpec as P

BF16, F32 = jnp.bfloat16, jnp.float32
MESH = pl.DeviceIdType.MESH

HALF = 128
M = 2 * HALF
NT = 1024
BLK = 32
MOVED = 48
KEPT = HALF - MOVED
PIECES = ((0, 0, HALF), (1, 0, HALF), (2, 0, HALF), (3, 0, KEPT), (3, KEPT, MOVED))
TERMS_AT = {3: (0, 1, 2), 4: (3,), 5: (4,), 6: (5,), 7: (6,)}
LAST = 3
ROUND = (16, 768)

ORDER = (("L", 0), ("L", 1), ("R", 0), ("L", 2), ("R", 1), ("R", 2), ("L", 3), ("R", 3))
SLOT = {k: s for s, k in enumerate(ORDER)}
FORWARD_MID = {1: 0, 4: 2, 5: 3}
FORWARD_END = {2: 1}


def kernel(
    x, w_gate, w_up, w_down, out,
    xs, wgu, wd, hid, term, local, to_sib, from_sib, to_far, from_far,
    load, early, far_recv, fwd_recv, sum_recv, sent, relay, relay_sem,
):
    me = lax.axis_index("tp")
    core = lax.rem(me, 2)
    sib = me + 1 - 2 * core
    far = lax.rem(me + 2, 4)
    dp, chip = lax.axis_index("dp"), lax.div(me, 2)
    giver = (core == 0) & (dp == 0) & (chip == 1)
    first_hop = (core == 0) & (dp == 1) & (chip == 1)
    second_hop = (core == 0) & (dp == 1) & (chip == 0)
    across = dp + chip - 2 * dp * chip
    steps = len(ORDER)
    tiles = wd.shape[0]
    chunks = x.shape[0] // HALF
    depth = x.shape[1]
    sent = sent.at[0]
    sib_recv = (early.at[0], early.at[1])
    fwd_recv = (fwd_recv.at[0], early.at[0], early.at[1], early.at[0])
    term_recv = tuple(far_recv.at[i] for i in range(4)) + (load.at[1],)

    def when(c, f):
        pl.when(c)(f)

    def remote(src, dst, send_sem, recv_sem, tp):
        return pltpu.make_async_remote_copy(
            src_ref=src, dst_ref=dst, send_sem=send_sem, recv_sem=recv_sem,
            device_id={"tp": tp}, device_id_type=MESH)

    def arrived(ref, sem):
        remote(ref, ref, sem, sem, far).wait_recv()

    def left(ref, sem):
        remote(ref, ref, sem, sem, far).wait_send()

    def slab(key, first, n):
        return xs.at[pl.ds(SLOT[key] * M + first, n)]

    def own(j):
        return pltpu.make_async_copy(x.at[pl.ds(j * HALF, HALF)], slab(("L", j), 0, HALF), sib_recv[0])

    def weights(n):
        c = pl.ds(n * NT, NT)
        return (pltpu.make_async_copy(w_gate.at[:, c], wgu.at[pl.ds(2 * n * depth, depth)], load.at[0]),
                pltpu.make_async_copy(w_up.at[:, c], wgu.at[pl.ds((2 * n + 1) * depth, depth)], load.at[0]))

    def weights_down(n):
        return pltpu.make_async_copy(w_down.at[:, pl.ds(n * NT, NT)], wd.at[n], load.at[1])

    def to_far_chip(p):
        j, r, n = PIECES[p]
        return remote(x.at[pl.ds(j * HALF + r, n)], slab(("R", j), r, n), sent, far_recv.at[j], far)

    def to_sibling(j):
        return remote(x.at[pl.ds(j * HALF, HALF)], slab(("L", j), HALF, HALF), sent, sib_recv[min(j, 1)], sib)

    def forward(p):
        i, r, n = PIECES[p]
        return remote(slab(("R", i), r, n), slab(("R", i), HALF + r, n), sent, fwd_recv[i], sib)

    def extra():
        return remote(slab(("L", LAST), HALF + KEPT, MOVED), slab(("R", LAST), HALF + KEPT, MOVED),
                      sent, far_recv.at[LAST], far)

    def extra_forward():
        return remote(slab(("R", LAST), HALF + KEPT, MOVED), slab(("R", LAST), KEPT, MOVED),
                      sent, fwd_recv[LAST], sib)

    round_rows = KEPT - ROUND[0]

    def over_y(src, dst, send_sem, recv_sem):
        return pltpu.make_async_remote_copy(
            src_ref=src, dst_ref=dst, send_sem=send_sem, recv_sem=recv_sem,
            device_id={"dp": 1 - dp}, device_id_type=MESH)

    def give():
        src = x.at[pl.ds(LAST * HALF + round_rows, ROUND[0]), pl.ds(0, ROUND[1])]
        return over_y(src, relay.at[0], sent, relay_sem.at[0])

    def relay_on():
        return remote(relay.at[0], relay.at[1], load.at[0], relay_sem.at[0], far)

    def hand_over():
        dst = xs.at[pl.ds(SLOT["R", LAST] * M + round_rows, ROUND[0]), pl.ds(0, ROUND[1])]
        return over_y(relay.at[1], dst, load.at[0], far_recv.at[LAST])

    def not_given():
        at, to = LAST * HALF, SLOT["R", LAST] * M
        rest = pl.ds(ROUND[1], depth - ROUND[1])
        return (remote(x.at[pl.ds(at, round_rows)], xs.at[pl.ds(to, round_rows)], sent, far_recv.at[LAST], far),
                remote(x.at[pl.ds(at + round_rows, ROUND[0]), rest],
                       xs.at[pl.ds(to + round_rows, ROUND[0]), rest], sent, far_recv.at[LAST], far))

    def term_copy(s):
        kind, i = ORDER[s]
        return remote(to_sib.at[s], from_sib.at[s], sent, term_recv[i if kind == "R" else chunks], sib)

    def sum_copy(p):
        i, r, n = PIECES[p]
        rows = pl.ds(i * HALF + r, n)
        return remote(to_far.at[rows], from_far.at[rows], sent, sum_recv.at[p // LAST_PIECE], far)

    barrier = pltpu.get_barrier_semaphore()
    pl.semaphore_signal(barrier, inc=1, device_id={"tp": far}, device_id_type=MESH)

    @pl.when(core == 1)
    def _():
        pl.semaphore_signal(barrier, inc=1, device_id={"tp": sib}, device_id_type=MESH)

    @pl.when((core == 0) & (across == 0))
    def _():
        pl.semaphore_signal(barrier, inc=1, device_id={"dp": 1 - dp}, device_id_type=MESH)

    pl.semaphore_wait(barrier, 2 - core + (1 - core) * across)
    for p in range(2):
        to_far_chip(p).start()
    when(giver, lambda: give().start())

    @pl.when(core == 0)
    def _():
        for j in range(chunks):
            to_sibling(j).start()

    for j in range(chunks):
        own(j).start()
    for n in range(tiles):
        for c in weights(n):
            c.start()
    for n in range(tiles):
        weights_down(n).start()
    arrived(xs.at[pl.ds(0, x.shape[0] + HALF)], sib_recv[0])

    @pl.when(core == 1)
    def _():
        for j in range(chunks):
            to_sibling(j).start()

    def pass_on(i):
        if i != LAST:
            arrived(slab(("R", i), 0, HALF), far_recv.at[i])
            forward(i).start()
            return

        @pl.when(core == 0)
        def _():
            arrived(slab(("R", i), 0, KEPT), far_recv.at[i])
            forward(LAST).start()

        @pl.when(core == 1)
        def _():
            arrived(slab(("R", i), 0, HALF + MOVED), far_recv.at[i])
            forward(LAST).start()
            forward(LAST_PIECE).start()
            extra_forward().start()

    def rows_in(k):
        kind, i = ORDER[k]
        if kind == "L":
            if i == 0:
                arrived(wgu, load.at[0])
        elif i != LAST:
            arrived(slab(("R", i), HALF, HALF), fwd_recv[i])
        else:
            @pl.when(core == 0)
            def _():
                arrived(slab(("R", i), 0, HALF + MOVED), fwd_recv[i])

            @pl.when(core == 1)
            def _():
                arrived(slab(("R", i), 0, KEPT), fwd_recv[i])

    def blocks(rows, f):
        def blk(r, _):
            f(pl.multiple_of(r * BLK, BLK))
            return 0
        lax.fori_loop(0, rows // BLK, blk, 0)

    def round_term(s):
        def blk(r):
            to_sib[s, pl.ds(r, BLK)] = term[lax.rem(s, 2), pl.ds(pl.multiple_of(HALF + r, BLK), BLK)].astype(BF16)
        blocks(HALF, blk)

    def keep_term(k):
        def blk(r):
            local[pl.ds(pl.multiple_of(ORDER[k][1] * HALF + r, BLK), BLK)] = term[k % 2, pl.ds(r, BLK)]
        blocks(HALF, blk)

    def add_sibling(j):
        def blk(r):
            at = pl.ds(pl.multiple_of(j * HALF + r, BLK), BLK)
            local[at] = local[at] + from_sib[SLOT["L", j], pl.ds(r, BLK)].astype(F32)
        blocks(HALF, blk)

    def chip_sum(k):
        i = ORDER[k][1]
        arrived(from_sib.at[k], term_recv[i])

        def blk(r):
            both = term[k % 2, pl.ds(r, BLK)] + from_sib[k, pl.ds(r, BLK)].astype(F32)
            to_far[pl.ds(pl.multiple_of(i * HALF + r, BLK), BLK)] = both.astype(BF16)
        blocks(HALF, blk)

    def start_sum(k):
        for p, (i, _, _) in enumerate(PIECES):
            if i == ORDER[k][1]:
                sum_copy(p).start()

    def step(s, _):
        for k in range(steps):
            when(s == k, lambda: rows_in(k))

        def gate_up(n, _):
            rows = xs.at[pl.ds(pl.multiple_of(s * M, M), M)]
            w = pl.multiple_of(2 * n * depth, depth)
            gate = jnp.dot(rows[...], wgu[pl.ds(w, depth)], preferred_element_type=F32)
            up = jnp.dot(rows[...], wgu[pl.ds(pl.multiple_of(w + depth, depth), depth)], preferred_element_type=F32)
            hid[:, pl.ds(pl.multiple_of(n * NT, NT), NT)] = (jax.nn.silu(gate) * up).astype(BF16)

            for k in range(1, steps):
                for t in TERMS_AT.get(k, ()):
                    when((s == k) & (n == 0), lambda: term_copy(t).start())
            return 0

        lax.fori_loop(0, tiles, gate_up, 0)

        @pl.when(s == 0)
        def _():
            arrived(wd, load.at[1])
            arrived(xs.at[pl.ds(0, (chunks - 1) * HALF)], sib_recv[1])

            @pl.when(first_hop)
            def _():
                arrived(relay.at[0], relay_sem.at[0])
                relay_on().start()

            to_far_chip(2).start()

            @pl.when(giver)
            def _():
                for c in not_given():
                    c.start()

            @pl.when(jnp.logical_not(giver))
            def _():
                to_far_chip(LAST).start()

            @pl.when(core == 1)
            def _():
                to_far_chip(LAST_PIECE).start()
                extra().start()

        @pl.when((s == 3) & second_hop)
        def _():
            arrived(relay.at[1], relay_sem.at[0])
            hand_over().start()

        for k in range(1, steps):
            if ORDER[k - 1][0] == "R":
                when(s == k, lambda: chip_sum(k - 1))
        for k, i in FORWARD_MID.items():
            when(s == k, lambda: pass_on(i))

        def down(n, _):
            cols = pl.ds(pl.multiple_of(n * NT, NT), NT)
            term[lax.rem(s, 2), :, cols] = jnp.dot(hid[...], wd[n], preferred_element_type=F32)
            for k in range(1, steps):
                if ORDER[k - 1][0] == "R":
                    when((s == k) & (n == 0), lambda: start_sum(k - 1))
            return 0

        lax.fori_loop(0, tiles, down, 0)

        round_term(s)
        for k in range(steps):
            if ORDER[k][0] == "L":
                when(s == k, lambda: keep_term(k))
        for k, i in FORWARD_END.items():
            when(s == k, lambda: pass_on(i))
        return 0

    lax.fori_loop(0, steps, step, 0)

    last = steps - 1
    arrived(from_sib.at[pl.ds(0, chunks)], term_recv[chunks])
    add_sibling(0)
    add_sibling(1)
    term_copy(last).start()
    add_sibling(2)
    chip_sum(last)
    add_sibling(3)
    start_sum(last)

    def finish(p):
        i, r, n = PIECES[p]
        rows = pl.ds(i * HALF + r, n)
        out[rows] = (local[rows] + from_far[rows].astype(F32)).astype(BF16)

    when(first_hop | second_hop, lambda: left(relay.at[0], load.at[0]))
    arrived(from_far.at[pl.ds(0, x.shape[0] - MOVED)], sum_recv.at[0])
    for p in range(LAST_PIECE):
        finish(p)
    arrived(from_far.at[pl.ds(0, MOVED)], sum_recv.at[1])
    finish(LAST_PIECE)
    rows = x.shape[0]
    for c, far_rows in enumerate((rows - MOVED, rows + MOVED)):
        total = 2 * (far_rows + rows) + steps * HALF
        when(core == c, lambda: left(wgu.at[pl.ds(0, total * depth // NT)], sent))


LAST_PIECE = len(PIECES) - 1


def solution(mesh):
    def step(x, w_gate, w_up, w_down):
        rows, d = x.shape
        f = w_gate.shape[1]
        chunks = rows // HALF
        steps = len(ORDER)
        dma = pltpu.SemaphoreType.DMA
        return pl.pallas_call(
            kernel,
            out_shape=pltpu.VMEM((rows, d), BF16),
            in_specs=[pl.BlockSpec(memory_space=pl.ANY)] * 4,
            out_specs=pl.BlockSpec(memory_space=pltpu.VMEM),
            scratch_shapes=[
                pltpu.VMEM((steps * M, d), BF16),
                pltpu.VMEM((2 * f // NT * d, NT), BF16),
                pltpu.VMEM((d // NT, f, NT), BF16),
                pltpu.VMEM((M, f), BF16),
                pltpu.VMEM((2, M, d), F32),
                pltpu.VMEM((rows, d), F32),
                pltpu.VMEM((steps, HALF, d), BF16),
                pltpu.VMEM((steps, HALF, d), BF16),
                pltpu.VMEM((rows, d), BF16),
                pltpu.VMEM((rows, d), BF16),
                dma((2,)),
                dma((2,)),
                dma((chunks,)),
                dma((1,)),
                dma((2,)),
                dma((1,)),
                pltpu.VMEM((2, *ROUND), BF16),
                dma((1,)),
            ],
            compiler_params=pltpu.CompilerParams(
                collective_id=0, has_side_effects=True, vmem_limit_bytes=63000000),
            name="mlp_ring",
        )(x, w_gate, w_up, w_down)

    return jax.shard_map(
        step,
        mesh=mesh,
        in_specs=(P(("dp", "tp"), None), P(None, "tp"), P(None, "tp"), P("tp", None)),
        out_specs=P(("dp", "tp"), None),
        check_vma=False,
    )
```

```python
import jax
import jax.numpy as jnp
from jax import lax
from jax.experimental import pallas as pl
from jax.experimental.pallas import tpu as pltpu
from jax.sharding import PartitionSpec as P

BF16, F32 = jnp.bfloat16, jnp.float32
MESH = pl.DeviceIdType.MESH

HALF = 128
M = 2 * HALF
NT = 1024
BLK = 32
MOVED = 48
KEPT = HALF - MOVED
PIECES = ((0, 0, HALF), (1, 0, HALF), (2, 0, HALF), (3, 0, KEPT), (3, KEPT, MOVED))
TERMS_AT = {3: (0, 1, 2), 4: (3,), 5: (4,), 6: (5,), 7: (6,)}
LAST = 3
ROUND = (16, 768)

ORDER = (("L", 0), ("L", 1), ("R", 0), ("L", 2), ("R", 1), ("R", 2), ("L", 3), ("R", 3))
SLOT = {k: s for s, k in enumerate(ORDER)}
FORWARD_MID = {1: 0, 4: 2, 5: 3}
FORWARD_END = {2: 1}


def kernel(
    x, w_gate, w_up, w_down, out,
    xs, wgu, wd, hid, term, local, to_sib, from_sib, to_far, from_far,
    load, early, far_recv, fwd_recv, sum_recv, sent, relay, relay_sem,
):
    me = lax.axis_index("tp")
    core = lax.rem(me, 2)
    sib = me + 1 - 2 * core
    far = lax.rem(me + 2, 4)
    dp, chip = lax.axis_index("dp"), lax.div(me, 2)
    giver = (core == 0) & (dp == 0) & (chip == 1)
    first_hop = (core == 0) & (dp == 1) & (chip == 1)
    second_hop = (core == 0) & (dp == 1) & (chip == 0)
    across = dp + chip - 2 * dp * chip
    steps = len(ORDER)
    tiles = wd.shape[0]
    chunks = x.shape[0] // HALF
    depth = x.shape[1]
    sent = sent.at[0]
    sib_recv = (early.at[0], early.at[1])
    fwd_recv = (fwd_recv.at[0], early.at[0], early.at[1], early.at[0])
    term_recv = tuple(far_recv.at[i] for i in range(4)) + (load.at[1],)

    def when(c, f):
        pl.when(c)(f)

    def remote(src, dst, send_sem, recv_sem, tp):
        return pltpu.make_async_remote_copy(
            src_ref=src, dst_ref=dst, send_sem=send_sem, recv_sem=recv_sem,
            device_id={"tp": tp}, device_id_type=MESH)

    def arrived(ref, sem):
        remote(ref, ref, sem, sem, far).wait_recv()

    def left(ref, sem):
        remote(ref, ref, sem, sem, far).wait_send()

    def slab(key, first, n):
        return xs.at[pl.ds(SLOT[key] * M + first, n)]

    def own(j):
        return pltpu.make_async_copy(x.at[pl.ds(j * HALF, HALF)], slab(("L", j), 0, HALF), load.at[0])

    def weights(n):
        c = pl.ds(n * NT, NT)
        return (pltpu.make_async_copy(w_gate.at[:, c], wgu.at[pl.ds(2 * n * depth, depth)], load.at[0]),
                pltpu.make_async_copy(w_up.at[:, c], wgu.at[pl.ds((2 * n + 1) * depth, depth)], load.at[0]))

    def weights_down(n):
        return pltpu.make_async_copy(w_down.at[:, pl.ds(n * NT, NT)], wd.at[n], load.at[1])

    def to_far_chip(p):
        j, r, n = PIECES[p]
        return remote(x.at[pl.ds(j * HALF + r, n)], slab(("R", j), r, n), sent, far_recv.at[j], far)

    def to_sibling(j):
        return remote(x.at[pl.ds(j * HALF, HALF)], slab(("L", j), HALF, HALF), sent, sib_recv[min(j, 1)], sib)

    def forward(p):
        i, r, n = PIECES[p]
        return remote(slab(("R", i), r, n), slab(("R", i), HALF + r, n), sent, fwd_recv[i], sib)

    def extra():
        return remote(slab(("L", LAST), HALF + KEPT, MOVED), slab(("R", LAST), HALF + KEPT, MOVED),
                      sent, far_recv.at[LAST], far)

    def extra_forward():
        return remote(slab(("R", LAST), HALF + KEPT, MOVED), slab(("R", LAST), KEPT, MOVED),
                      sent, fwd_recv[LAST], sib)

    round_rows = KEPT - ROUND[0]

    def over_y(src, dst, send_sem, recv_sem):
        return pltpu.make_async_remote_copy(
            src_ref=src, dst_ref=dst, send_sem=send_sem, recv_sem=recv_sem,
            device_id={"dp": 1 - dp}, device_id_type=MESH)

    def give():
        src = x.at[pl.ds(LAST * HALF + round_rows, ROUND[0]), pl.ds(0, ROUND[1])]
        return over_y(src, relay.at[0], sent, relay_sem.at[0])

    def relay_on():
        return remote(relay.at[0], relay.at[1], load.at[0], relay_sem.at[0], far)

    def hand_over():
        dst = xs.at[pl.ds(SLOT["R", LAST] * M + round_rows, ROUND[0]), pl.ds(0, ROUND[1])]
        return over_y(relay.at[1], dst, load.at[0], far_recv.at[LAST])

    def not_given():
        at, to = LAST * HALF, SLOT["R", LAST] * M
        rest = pl.ds(ROUND[1], depth - ROUND[1])
        return (remote(x.at[pl.ds(at, round_rows)], xs.at[pl.ds(to, round_rows)], sent, far_recv.at[LAST], far),
                remote(x.at[pl.ds(at + round_rows, ROUND[0]), rest],
                       xs.at[pl.ds(to + round_rows, ROUND[0]), rest], sent, far_recv.at[LAST], far))

    def term_copy(s):
        kind, i = ORDER[s]
        return remote(to_sib.at[s], from_sib.at[s], sent, term_recv[i if kind == "R" else chunks], sib)

    def sum_copy(p):
        i, r, n = PIECES[p]
        rows = pl.ds(i * HALF + r, n)
        return remote(to_far.at[rows], from_far.at[rows], sent, sum_recv.at[p // LAST_PIECE], far)

    barrier = pltpu.get_barrier_semaphore()
    pl.semaphore_signal(barrier, inc=1, device_id={"tp": far}, device_id_type=MESH)

    @pl.when(core == 1)
    def _():
        pl.semaphore_signal(barrier, inc=1, device_id={"tp": sib}, device_id_type=MESH)

    @pl.when((core == 0) & (across == 0))
    def _():
        pl.semaphore_signal(barrier, inc=1, device_id={"dp": 1 - dp}, device_id_type=MESH)

    pl.semaphore_wait(barrier, 2 - core + (1 - core) * across)
    for p in range(2):
        to_far_chip(p).start()
    when(giver, lambda: give().start())

    @pl.when(core == 0)
    def _():
        for j in range(chunks):
            to_sibling(j).start()

    for j in range(chunks):
        own(j).start()
    for n in range(tiles):
        for c in weights(n):
            c.start()
    for n in range(tiles):
        weights_down(n).start()
    arrived(xs.at[pl.ds(0, HALF)], sib_recv[0])

    @pl.when(core == 1)
    def _():
        for j in range(chunks):
            to_sibling(j).start()

    def pass_on(i):
        if i != LAST:
            arrived(slab(("R", i), 0, HALF), far_recv.at[i])
            forward(i).start()
            return

        @pl.when(core == 0)
        def _():
            arrived(slab(("R", i), 0, KEPT), far_recv.at[i])
            forward(LAST).start()

        @pl.when(core == 1)
        def _():
            arrived(slab(("R", i), 0, HALF + MOVED), far_recv.at[i])
            forward(LAST).start()
            forward(LAST_PIECE).start()
            extra_forward().start()

    def rows_in(k):
        kind, i = ORDER[k]
        if kind == "L":
            if i == 0:
                arrived(xs.at[pl.ds(0, (chunks - 1) * HALF)], sib_recv[1])
                arrived(wgu, load.at[0])
                arrived(xs.at[pl.ds(0, x.shape[0])], load.at[0])
        elif i != LAST:
            arrived(slab(("R", i), HALF, HALF), fwd_recv[i])
        else:
            @pl.when(core == 0)
            def _():
                arrived(slab(("R", i), 0, HALF + MOVED), fwd_recv[i])

            @pl.when(core == 1)
            def _():
                arrived(slab(("R", i), 0, KEPT), fwd_recv[i])

    def blocks(rows, f):
        def blk(r, _):
            f(pl.multiple_of(r * BLK, BLK))
            return 0
        lax.fori_loop(0, rows // BLK, blk, 0)

    def round_term(s):
        def blk(r):
            to_sib[s, pl.ds(r, BLK)] = term[lax.rem(s, 2), pl.ds(pl.multiple_of(HALF + r, BLK), BLK)].astype(BF16)
        blocks(HALF, blk)

    def keep_term(k):
        def blk(r):
            local[pl.ds(pl.multiple_of(ORDER[k][1] * HALF + r, BLK), BLK)] = term[k % 2, pl.ds(r, BLK)]
        blocks(HALF, blk)

    def add_sibling(j):
        def blk(r):
            at = pl.ds(pl.multiple_of(j * HALF + r, BLK), BLK)
            local[at] = local[at] + from_sib[SLOT["L", j], pl.ds(r, BLK)].astype(F32)
        blocks(HALF, blk)

    def chip_sum(k):
        i = ORDER[k][1]
        arrived(from_sib.at[k], term_recv[i])

        def blk(r):
            both = term[k % 2, pl.ds(r, BLK)] + from_sib[k, pl.ds(r, BLK)].astype(F32)
            to_far[pl.ds(pl.multiple_of(i * HALF + r, BLK), BLK)] = both.astype(BF16)
        blocks(HALF, blk)

    def start_sum(k):
        for p, (i, _, _) in enumerate(PIECES):
            if i == ORDER[k][1]:
                sum_copy(p).start()

    def step(s, _):
        for k in range(steps):
            when(s == k, lambda: rows_in(k))

        def gate_up(n, _):
            rows = xs.at[pl.ds(pl.multiple_of(s * M, M), M)]
            w = pl.multiple_of(2 * n * depth, depth)
            gate = jnp.dot(rows[...], wgu[pl.ds(w, depth)], preferred_element_type=F32)
            up = jnp.dot(rows[...], wgu[pl.ds(pl.multiple_of(w + depth, depth), depth)], preferred_element_type=F32)
            hid[:, pl.ds(pl.multiple_of(n * NT, NT), NT)] = (jax.nn.silu(gate) * up).astype(BF16)

            for k in range(1, steps):
                for t in TERMS_AT.get(k, ()):
                    when((s == k) & (n == 0), lambda: term_copy(t).start())
            return 0

        lax.fori_loop(0, tiles, gate_up, 0)

        @pl.when(s == 0)
        def _():
            arrived(wd, load.at[1])

            @pl.when(first_hop)
            def _():
                arrived(relay.at[0], relay_sem.at[0])
                relay_on().start()

            to_far_chip(2).start()

            @pl.when(giver)
            def _():
                for c in not_given():
                    c.start()

            @pl.when(jnp.logical_not(giver))
            def _():
                to_far_chip(LAST).start()

            @pl.when(core == 1)
            def _():
                to_far_chip(LAST_PIECE).start()
                extra().start()

        @pl.when((s == 3) & second_hop)
        def _():
            arrived(relay.at[1], relay_sem.at[0])
            hand_over().start()

        for k in range(1, steps):
            if ORDER[k - 1][0] == "R":
                when(s == k, lambda: chip_sum(k - 1))
        for k, i in FORWARD_MID.items():
            when(s == k, lambda: pass_on(i))

        def down(n, _):
            cols = pl.ds(pl.multiple_of(n * NT, NT), NT)
            term[lax.rem(s, 2), :, cols] = jnp.dot(hid[...], wd[n], preferred_element_type=F32)
            for k in range(1, steps):
                if ORDER[k - 1][0] == "R":
                    when((s == k) & (n == 0), lambda: start_sum(k - 1))
            return 0

        lax.fori_loop(0, tiles, down, 0)

        round_term(s)
        for k in range(steps):
            if ORDER[k][0] == "L":
                when(s == k, lambda: keep_term(k))
        for k, i in FORWARD_END.items():
            when(s == k, lambda: pass_on(i))
        return 0

    lax.fori_loop(0, steps, step, 0)

    last = steps - 1
    arrived(from_sib.at[pl.ds(0, chunks)], term_recv[chunks])
    add_sibling(0)
    add_sibling(1)
    term_copy(last).start()
    add_sibling(2)
    chip_sum(last)
    add_sibling(3)
    start_sum(last)

    def finish(p):
        i, r, n = PIECES[p]
        rows = pl.ds(i * HALF + r, n)
        out[rows] = (local[rows] + from_far[rows].astype(F32)).astype(BF16)

    when(first_hop | second_hop, lambda: left(relay.at[0], load.at[0]))
    arrived(from_far.at[pl.ds(0, x.shape[0] - MOVED)], sum_recv.at[0])
    for p in range(LAST_PIECE):
        finish(p)
    arrived(from_far.at[pl.ds(0, MOVED)], sum_recv.at[1])
    finish(LAST_PIECE)
    rows = x.shape[0]
    for c, far_rows in enumerate((rows - MOVED, rows + MOVED)):
        total = 2 * (far_rows + rows) + steps * HALF
        when(core == c, lambda: left(wgu.at[pl.ds(0, total * depth // NT)], sent))


LAST_PIECE = len(PIECES) - 1


def solution(mesh):
    def step(x, w_gate, w_up, w_down):
        rows, d = x.shape
        f = w_gate.shape[1]
        chunks = rows // HALF
        steps = len(ORDER)
        dma = pltpu.SemaphoreType.DMA
        return pl.pallas_call(
            kernel,
            out_shape=pltpu.VMEM((rows, d), BF16),
            in_specs=[pl.BlockSpec(memory_space=pl.ANY)] * 4,
            out_specs=pl.BlockSpec(memory_space=pltpu.VMEM),
            scratch_shapes=[
                pltpu.VMEM((steps * M, d), BF16),
                pltpu.VMEM((2 * f // NT * d, NT), BF16),
                pltpu.VMEM((d // NT, f, NT), BF16),
                pltpu.VMEM((M, f), BF16),
                pltpu.VMEM((2, M, d), F32),
                pltpu.VMEM((rows, d), F32),
                pltpu.VMEM((steps, HALF, d), BF16),
                pltpu.VMEM((steps, HALF, d), BF16),
                pltpu.VMEM((rows, d), BF16),
                pltpu.VMEM((rows, d), BF16),
                dma((2,)),
                dma((2,)),
                dma((chunks,)),
                dma((1,)),
                dma((2,)),
                dma((1,)),
                pltpu.VMEM((2, *ROUND), BF16),
                dma((1,)),
            ],
            compiler_params=pltpu.CompilerParams(
                collective_id=0, has_side_effects=True, vmem_limit_bytes=63000000),
            name="mlp_ring",
        )(x, w_gate, w_up, w_down)

    return jax.shard_map(
        step,
        mesh=mesh,
        in_specs=(P(("dp", "tp"), None), P(None, "tp"), P(None, "tp"), P("tp", None)),
        out_specs=P(("dp", "tp"), None),
        check_vma=False,
    )
```

```python
import jax
import jax.numpy as jnp
from jax import lax
from jax.experimental import pallas as pl
from jax.experimental.pallas import tpu as pltpu
from jax.sharding import PartitionSpec as P

BF16, F32 = jnp.bfloat16, jnp.float32
MESH = pl.DeviceIdType.MESH

HALF = 128
M = 2 * HALF
NT = 1024
BLK = 32
MOVED = 48
KEPT = HALF - MOVED
PIECES = ((0, 0, HALF), (1, 0, HALF), (2, 0, HALF), (3, 0, KEPT), (3, KEPT, MOVED))
TERMS_AT = {3: (0, 1, 2), 4: (3,), 5: (4,), 6: (5,), 7: (6,)}
SUMS = ((0, 0, HALF), (1, 0, HALF), (2, 0, HALF), (3, 0, HALF - 16), (3, HALF - 16, 16))
LAST = 3
ROUND = (16, 768)

ORDER = (("L", 0), ("L", 1), ("R", 0), ("L", 2), ("R", 1), ("R", 2), ("L", 3), ("R", 3))
SLOT = {k: s for s, k in enumerate(ORDER)}
FORWARD_MID = {1: 0, 4: 2, 5: 3}
FORWARD_END = {2: 1}


def kernel(
    x, w_gate, w_up, w_down, out,
    xs, wgu, wd, hid, term, local, to_sib, from_sib, to_far, from_far,
    load, early, far_recv, sum_first, sent, relay, relay_sem,
):
    me = lax.axis_index("tp")
    core = lax.rem(me, 2)
    sib = me + 1 - 2 * core
    far = lax.rem(me + 2, 4)
    dp, chip = lax.axis_index("dp"), lax.div(me, 2)
    giver = (core == 0) & (dp == 0) & (chip == 1)
    first_hop = (core == 0) & (dp == 1) & (chip == 1)
    second_hop = (core == 0) & (dp == 1) & (chip == 0)
    across = dp + chip - 2 * dp * chip
    steps = len(ORDER)
    tiles = wd.shape[0]
    chunks = x.shape[0] // HALF
    depth = x.shape[1]
    sent = sent.at[0]
    sib_recv = (early.at[0], early.at[1])
    fwd_recv = (early.at[0], early.at[1], early.at[0], early.at[1])
    term_recv = tuple(far_recv.at[i] for i in range(4)) + (load.at[1],)
    sum_recv = (sum_first.at[0], load.at[0])

    def when(c, f):
        pl.when(c)(f)

    def remote(src, dst, send_sem, recv_sem, tp):
        return pltpu.make_async_remote_copy(
            src_ref=src, dst_ref=dst, send_sem=send_sem, recv_sem=recv_sem,
            device_id={"tp": tp}, device_id_type=MESH)

    def arrived(ref, sem):
        remote(ref, ref, sem, sem, far).wait_recv()

    def left(ref, sem):
        remote(ref, ref, sem, sem, far).wait_send()

    def slab(key, first, n):
        return xs.at[pl.ds(SLOT[key] * M + first, n)]

    def own(j):
        return pltpu.make_async_copy(x.at[pl.ds(j * HALF, HALF)], slab(("L", j), 0, HALF), sib_recv[0])

    def weights(n):
        c = pl.ds(n * NT, NT)
        return (pltpu.make_async_copy(w_gate.at[:, c], wgu.at[pl.ds(2 * n * depth, depth)], load.at[0]),
                pltpu.make_async_copy(w_up.at[:, c], wgu.at[pl.ds((2 * n + 1) * depth, depth)], load.at[0]))

    def weights_down(n):
        return pltpu.make_async_copy(w_down.at[:, pl.ds(n * NT, NT)], wd.at[n], load.at[1])

    def to_far_chip(p):
        j, r, n = PIECES[p]
        return remote(x.at[pl.ds(j * HALF + r, n)], slab(("R", j), r, n), sent, far_recv.at[j], far)

    def to_sibling(j):
        return remote(x.at[pl.ds(j * HALF, HALF)], slab(("L", j), HALF, HALF), sent, sib_recv[min(j, 1)], sib)

    def forward(p):
        i, r, n = PIECES[p]
        return remote(slab(("R", i), r, n), slab(("R", i), HALF + r, n), sent, fwd_recv[i], sib)

    def extra():
        return remote(slab(("L", LAST), HALF + KEPT, MOVED), slab(("R", LAST), HALF + KEPT, MOVED),
                      sent, far_recv.at[LAST], far)

    def extra_forward():
        return remote(slab(("R", LAST), HALF + KEPT, MOVED), slab(("R", LAST), KEPT, MOVED),
                      sent, fwd_recv[LAST], sib)

    round_rows = KEPT - ROUND[0]

    def over_y(src, dst, send_sem, recv_sem):
        return pltpu.make_async_remote_copy(
            src_ref=src, dst_ref=dst, send_sem=send_sem, recv_sem=recv_sem,
            device_id={"dp": 1 - dp}, device_id_type=MESH)

    def give():
        src = x.at[pl.ds(LAST * HALF + round_rows, ROUND[0]), pl.ds(0, ROUND[1])]
        return over_y(src, relay.at[0], sent, relay_sem.at[0])

    def relay_on():
        return remote(relay.at[0], relay.at[1], relay_sem.at[0], relay_sem.at[0], far)

    def hand_over():
        dst = xs.at[pl.ds(SLOT["R", LAST] * M + round_rows, ROUND[0]), pl.ds(0, ROUND[1])]
        return over_y(relay.at[1], dst, relay_sem.at[0], far_recv.at[LAST])

    def not_given():
        at, to = LAST * HALF, SLOT["R", LAST] * M
        rest = pl.ds(ROUND[1], depth - ROUND[1])
        return (remote(x.at[pl.ds(at, round_rows)], xs.at[pl.ds(to, round_rows)], sent, far_recv.at[LAST], far),
                remote(x.at[pl.ds(at + round_rows, ROUND[0]), rest],
                       xs.at[pl.ds(to + round_rows, ROUND[0]), rest], sent, far_recv.at[LAST], far))

    def term_copy(s):
        kind, i = ORDER[s]
        return remote(to_sib.at[s], from_sib.at[s], sent, term_recv[i if kind == "R" else chunks], sib)

    def sum_copy(p):
        i, r, n = SUMS[p]
        rows = pl.ds(i * HALF + r, n)
        return remote(to_far.at[rows], from_far.at[rows], sent, sum_recv[p // LAST_PIECE], far)

    barrier = pltpu.get_barrier_semaphore()
    pl.semaphore_signal(barrier, inc=1, device_id={"tp": far}, device_id_type=MESH)

    @pl.when(core == 1)
    def _():
        pl.semaphore_signal(barrier, inc=1, device_id={"tp": sib}, device_id_type=MESH)

    @pl.when((core == 0) & (across == 0))
    def _():
        pl.semaphore_signal(barrier, inc=1, device_id={"dp": 1 - dp}, device_id_type=MESH)

    pl.semaphore_wait(barrier, 2 - core + (1 - core) * across)
    for p in range(2):
        to_far_chip(p).start()
    when(giver, lambda: give().start())

    when(core == 0, lambda: to_sibling(0).start())
    for j in range(chunks):
        own(j).start()
    for n in range(tiles):
        for c in weights(n):
            c.start()
    for n in range(tiles):
        weights_down(n).start()
    arrived(xs.at[pl.ds(0, x.shape[0] + HALF)], sib_recv[0])

    when(core == 1, lambda: to_sibling(0).start())
    for j in range(1, chunks):
        to_sibling(j).start()

    def pass_on(i):
        if i != LAST:
            arrived(slab(("R", i), 0, HALF), far_recv.at[i])
            forward(i).start()
            return

        @pl.when(core == 0)
        def _():
            arrived(slab(("R", i), 0, KEPT), far_recv.at[i])
            forward(LAST).start()

        @pl.when(core == 1)
        def _():
            arrived(slab(("R", i), 0, HALF + MOVED), far_recv.at[i])
            forward(LAST).start()
            forward(LAST_PIECE).start()
            extra_forward().start()

    def rows_in(k):
        kind, i = ORDER[k]
        if kind == "L":
            if i == 0:
                arrived(wgu, load.at[0])
        elif i != LAST:
            arrived(slab(("R", i), HALF, HALF), fwd_recv[i])
        else:
            @pl.when(core == 0)
            def _():
                arrived(slab(("R", i), 0, HALF + MOVED), fwd_recv[i])

            @pl.when(core == 1)
            def _():
                arrived(slab(("R", i), 0, KEPT), fwd_recv[i])

    def blocks(rows, f):
        def blk(r, _):
            f(pl.multiple_of(r * BLK, BLK))
            return 0
        lax.fori_loop(0, rows // BLK, blk, 0)

    def round_term(s):
        def blk(r):
            to_sib[s, pl.ds(r, BLK)] = term[lax.rem(s, 2), pl.ds(pl.multiple_of(HALF + r, BLK), BLK)].astype(BF16)
        blocks(HALF, blk)

    def keep_term(k):
        def blk(r):
            local[pl.ds(pl.multiple_of(ORDER[k][1] * HALF + r, BLK), BLK)] = term[k % 2, pl.ds(r, BLK)]
        blocks(HALF, blk)

    def add_sibling(j):
        def blk(r):
            at = pl.ds(pl.multiple_of(j * HALF + r, BLK), BLK)
            local[at] = local[at] + from_sib[SLOT["L", j], pl.ds(r, BLK)].astype(F32)
        blocks(HALF, blk)

    def chip_sum(k):
        i = ORDER[k][1]
        arrived(from_sib.at[k], term_recv[i])

        def blk(r):
            both = term[k % 2, pl.ds(r, BLK)] + from_sib[k, pl.ds(r, BLK)].astype(F32)
            to_far[pl.ds(pl.multiple_of(i * HALF + r, BLK), BLK)] = both.astype(BF16)
        blocks(HALF, blk)

    def start_sum(k):
        for p, (i, _, _) in enumerate(SUMS):
            if i == ORDER[k][1]:
                sum_copy(p).start()

    def step(s, _):
        for k in range(steps):
            when(s == k, lambda: rows_in(k))

        def gate_up(n, _):
            rows = xs.at[pl.ds(pl.multiple_of(s * M, M), M)]
            w = pl.multiple_of(2 * n * depth, depth)
            gate = jnp.dot(rows[...], wgu[pl.ds(w, depth)], preferred_element_type=F32)
            up = jnp.dot(rows[...], wgu[pl.ds(pl.multiple_of(w + depth, depth), depth)], preferred_element_type=F32)
            hid[:, pl.ds(pl.multiple_of(n * NT, NT), NT)] = (jax.nn.silu(gate) * up).astype(BF16)

            for k in range(1, steps):
                for t in TERMS_AT.get(k, ()):
                    when((s == k) & (n == 0), lambda: term_copy(t).start())
            return 0

        lax.fori_loop(0, tiles, gate_up, 0)

        @pl.when(s == 0)
        def _():
            arrived(wd, load.at[1])
            arrived(xs.at[pl.ds(0, (chunks - 1) * HALF)], sib_recv[1])

            @pl.when(first_hop)
            def _():
                arrived(relay.at[0], relay_sem.at[0])
                relay_on().start()

            to_far_chip(2).start()

            @pl.when(giver)
            def _():
                for c in not_given():
                    c.start()

            @pl.when(jnp.logical_not(giver))
            def _():
                to_far_chip(LAST).start()

            @pl.when(core == 1)
            def _():
                to_far_chip(LAST_PIECE).start()
                extra().start()

        @pl.when((s == 3) & second_hop)
        def _():
            arrived(relay.at[1], relay_sem.at[0])
            hand_over().start()

        for k in range(1, steps):
            if ORDER[k - 1][0] == "R":
                when(s == k, lambda: chip_sum(k - 1))
        for k, i in FORWARD_MID.items():
            when(s == k, lambda: pass_on(i))

        def down(n, _):
            cols = pl.ds(pl.multiple_of(n * NT, NT), NT)
            term[lax.rem(s, 2), :, cols] = jnp.dot(hid[...], wd[n], preferred_element_type=F32)
            for k in range(1, steps):
                if ORDER[k - 1][0] == "R":
                    when((s == k) & (n == 0), lambda: start_sum(k - 1))
            return 0

        lax.fori_loop(0, tiles, down, 0)

        round_term(s)
        for k in range(steps):
            if ORDER[k][0] == "L":
                when(s == k, lambda: keep_term(k))
        for k, i in FORWARD_END.items():
            when(s == k, lambda: pass_on(i))
        return 0

    lax.fori_loop(0, steps, step, 0)

    last = steps - 1
    arrived(from_sib.at[pl.ds(0, chunks)], term_recv[chunks])
    add_sibling(0)
    add_sibling(1)
    term_copy(last).start()
    add_sibling(2)
    chip_sum(last)
    add_sibling(3)
    start_sum(last)

    def finish(p):
        i, r, n = SUMS[p]
        rows = pl.ds(i * HALF + r, n)
        out[rows] = (local[rows] + from_far[rows].astype(F32)).astype(BF16)

    when(first_hop | second_hop, lambda: left(relay.at[0], relay_sem.at[0]))
    arrived(from_far.at[pl.ds(0, x.shape[0] - SUMS[-1][2])], sum_recv[0])
    for p in range(LAST_PIECE):
        finish(p)
    arrived(from_far.at[pl.ds(0, SUMS[-1][2])], sum_recv[1])
    finish(LAST_PIECE)
    rows = x.shape[0]
    for c, far_rows in enumerate((rows - MOVED, rows + MOVED)):
        total = 2 * (far_rows + rows) + steps * HALF
        when(core == c, lambda: left(wgu.at[pl.ds(0, total * depth // NT)], sent))


LAST_PIECE = len(PIECES) - 1


def solution(mesh):
    def step(x, w_gate, w_up, w_down):
        rows, d = x.shape
        f = w_gate.shape[1]
        chunks = rows // HALF
        steps = len(ORDER)
        dma = pltpu.SemaphoreType.DMA
        return pl.pallas_call(
            kernel,
            out_shape=pltpu.VMEM((rows, d), BF16),
            in_specs=[pl.BlockSpec(memory_space=pl.ANY)] * 4,
            out_specs=pl.BlockSpec(memory_space=pltpu.VMEM),
            scratch_shapes=[
                pltpu.VMEM((steps * M, d), BF16),
                pltpu.VMEM((2 * f // NT * d, NT), BF16),
                pltpu.VMEM((d // NT, f, NT), BF16),
                pltpu.VMEM((M, f), BF16),
                pltpu.VMEM((2, M, d), F32),
                pltpu.VMEM((rows, d), F32),
                pltpu.VMEM((steps, HALF, d), BF16),
                pltpu.VMEM((steps, HALF, d), BF16),
                pltpu.VMEM((rows, d), BF16),
                pltpu.VMEM((rows, d), BF16),
                dma((2,)),
                dma((2,)),
                dma((chunks,)),
                dma((1,)),
                dma((1,)),
                pltpu.VMEM((2, *ROUND), BF16),
                dma((1,)),
            ],
            compiler_params=pltpu.CompilerParams(
                collective_id=0, has_side_effects=True, vmem_limit_bytes=63000000),
            name="mlp_ring",
        )(x, w_gate, w_up, w_down)

    return jax.shard_map(
        step,
        mesh=mesh,
        in_specs=(P(("dp", "tp"), None), P(None, "tp"), P(None, "tp"), P("tp", None)),
        out_specs=P(("dp", "tp"), None),
        check_vma=False,
    )
```
